16 devices in a mesh: dp: 2 (over y, z), tp: 8 (over x, core).
Axes of the slice: x: 4, y: 2, z: 1, core: 2. Of those that a mesh axis runs over, the one named last changes fastest.
The devices are a block of a 4x4x8 slice.
Arguments:
- hidden: bfloat16 [2048, 4544], P(('dp', 'tp')), parts along dimension 0
- positions: int32 [2048], P(('dp', 'tp')), parts along dimension 0
- ln_gamma: float32 [2, 4544], replicated
- ln_beta: float32 [2, 4544], replicated
- w_qkv: bfloat16 [2, 4544, 4672], replicated
- w_out: bfloat16 [2, 4544, 4544], replicated
- w_up: bfloat16 [2, 4544, 18176], P(None, None, 'tp')
- w_down: bfloat16 [2, 18176, 4544], P(None, 'tp')
- k_cache: bfloat16 [2, 2048, 256, 64], P(None, ('dp', 'tp')), parts along dimension 1
- v_cache: bfloat16 [2, 2048, 256, 64], P(None, ('dp', 'tp')), parts along dimension 1
Outputs:
- output 1: bfloat16 [2048, 4544], P(('dp', 'tp')), parts along dimension 0
- output 2: bfloat16 [2, 2048, 256, 64], P(None, ('dp', 'tp')), parts along dimension 1
- output 3: bfloat16 [2, 2048, 256, 64], P(None, ('dp', 'tp')), parts along dimension 1
There are 2 independent parts. The reference program is written for one: setup_inputs(seed, part) draws one part's arguments, and reference() takes and returns one part's arrays. A program takes and returns all parts, laid end to end along the dimension named above; an argument that names none is the same for every part.
All inputs are finite; a program needn't handle non-finite values.
Results may differ from the reference program's by a relative error of at most 0.0126439.
Values are sent between devices in bfloat16 or wider.
A program may use at most 768 MiB of HBM per device.

```python
import jax
import jax.numpy as jnp
from jax import lax

D_MODEL = 4544
NUM_HEADS = 71
HEAD_DIM = 64
FF_DIM = 18176
SEQ_LEN = 256
ROWS_DEV = 128
GROUP_SIZE = 8
NUM_LAYERS = 2

ATT_WIDTH = NUM_HEADS * HEAD_DIM
QKV_WIDTH = ATT_WIDTH + 2 * HEAD_DIM
GROUP_ROWS = ROWS_DEV * GROUP_SIZE
LN_EPS = 1e-5
ROPE_BASE = 10000.0


def setup_inputs(seed: int = 0, part: int = 0) -> dict:
    base_key = jax.random.key(seed)
    shared_keys = jax.random.split(base_key, 6)
    part_key = jax.random.fold_in(base_key, part)
    part_keys = jax.random.split(part_key, 6)
    hidden = jax.random.normal(part_keys[0], (GROUP_ROWS, D_MODEL), jnp.float32)
    drawn_pos = jax.random.randint(part_keys[1], (GROUP_ROWS,), 0, SEQ_LEN, jnp.int32)
    full_row = jax.random.randint(part_keys[2], (), 0, GROUP_ROWS, jnp.int32)
    positions = jnp.where(jnp.arange(GROUP_ROWS, dtype=jnp.int32) == full_row, SEQ_LEN - 1, drawn_pos).astype(jnp.int32)
    cache_shape = (NUM_LAYERS, GROUP_ROWS, SEQ_LEN, HEAD_DIM)
    k_cache = jax.random.normal(part_keys[3], cache_shape, jnp.float32)
    v_mean = jax.random.normal(part_keys[4], (NUM_LAYERS, GROUP_ROWS, 1, HEAD_DIM), jnp.float32)
    v_cache = v_mean + jax.random.normal(part_keys[5], cache_shape, jnp.float32)
    ln_gamma = 1.0 + 0.5 * jax.random.normal(shared_keys[0], (NUM_LAYERS, D_MODEL), jnp.float32)
    ln_beta = 0.5 * jax.random.normal(shared_keys[1], (NUM_LAYERS, D_MODEL), jnp.float32)
    w_qkv = jax.random.normal(shared_keys[2], (NUM_LAYERS, D_MODEL, QKV_WIDTH), jnp.float32) * D_MODEL ** -0.5
    w_out = jax.random.normal(shared_keys[3], (NUM_LAYERS, ATT_WIDTH, D_MODEL), jnp.float32) * ATT_WIDTH ** -0.5
    w_up = jax.random.normal(shared_keys[4], (NUM_LAYERS, D_MODEL, FF_DIM), jnp.float32) * D_MODEL ** -0.5
    w_down = jax.random.normal(shared_keys[5], (NUM_LAYERS, FF_DIM, D_MODEL), jnp.float32) * FF_DIM ** -0.5
    return {
        'hidden': hidden.astype(jnp.bfloat16),
        'positions': positions,
        'ln_gamma': ln_gamma,
        'ln_beta': ln_beta,
        'w_qkv': w_qkv.astype(jnp.bfloat16),
        'w_out': w_out.astype(jnp.bfloat16),
        'w_up': w_up.astype(jnp.bfloat16),
        'w_down': w_down.astype(jnp.bfloat16),
        'k_cache': k_cache.astype(jnp.bfloat16),
        'v_cache': v_cache.astype(jnp.bfloat16),
    }


def layer_norm(rows_in, gamma_row, beta_row):
    values = rows_in.astype(jnp.float32)
    row_mean = jnp.mean(values, axis=-1, keepdims=True)
    centered = values - row_mean
    variance = jnp.mean(centered * centered, axis=-1, keepdims=True)
    return (centered * lax.rsqrt(variance + LN_EPS) * gamma_row + beta_row).astype(jnp.bfloat16)


def rotary(vectors, positions):
    half_dim = HEAD_DIM // 2
    inv_freq = 1.0 / (ROPE_BASE ** (jnp.arange(half_dim, dtype=jnp.float32) * (2.0 / HEAD_DIM)))
    angles = positions.astype(jnp.float32)[:, None] * inv_freq[None, :]
    cos_table = jnp.cos(angles)[:, None, :]
    sin_table = jnp.sin(angles)[:, None, :]
    first_half = vectors[..., :half_dim]
    second_half = vectors[..., half_dim:]
    return jnp.concatenate([first_half * cos_table - second_half * sin_table, second_half * cos_table + first_half * sin_table], axis=-1)


def attend_block(block):
    qkv_rows, positions, k_rows, v_rows = block
    rows_n = qkv_rows.shape[0]
    qkv_float = qkv_rows.astype(jnp.float32)
    query_rot = rotary(qkv_float[:, :ATT_WIDTH].reshape(rows_n, NUM_HEADS, HEAD_DIM), positions).astype(jnp.bfloat16)
    key_rot = rotary(qkv_float[:, ATT_WIDTH:ATT_WIDTH + HEAD_DIM].reshape(rows_n, 1, HEAD_DIM), positions).astype(jnp.bfloat16)
    value_new = qkv_rows[:, None, ATT_WIDTH + HEAD_DIM:]
    seq_ids = jnp.arange(SEQ_LEN, dtype=jnp.int32)
    write_mask = seq_ids[None, :, None] == positions[:, None, None]
    k_upd = jnp.where(write_mask, key_rot, k_rows)
    v_upd = jnp.where(write_mask, value_new, v_rows)
    scores = jnp.einsum('bhd,bsd->bhs', query_rot.astype(jnp.float32), k_upd.astype(jnp.float32)) * (HEAD_DIM ** -0.5)
    scores = jnp.where(seq_ids[None, None, :] <= positions[:, None, None], scores, -1e30)
    probabilities = jax.nn.softmax(scores, axis=-1).astype(jnp.bfloat16)
    context = jnp.einsum('bhs,bsd->bhd', probabilities.astype(jnp.float32), v_upd.astype(jnp.float32))
    return context.astype(jnp.bfloat16).reshape(rows_n, ATT_WIDTH), k_upd, v_upd


def reference(hidden, positions, ln_gamma, ln_beta, w_qkv, w_out, w_up, w_down, k_cache, v_cache):
    def layer_step(hidden_state, layer_args):
        gamma_row, beta_row, qkv_weight, out_weight, up_weight, down_weight, k_layer, v_layer = layer_args
        normed = layer_norm(hidden_state, gamma_row, beta_row)
        qkv_rows = jnp.dot(normed, qkv_weight, preferred_element_type=jnp.float32).astype(jnp.bfloat16)
        blocks = (
            qkv_rows.reshape(GROUP_SIZE, ROWS_DEV, QKV_WIDTH),
            positions.reshape(GROUP_SIZE, ROWS_DEV),
            k_layer.reshape(GROUP_SIZE, ROWS_DEV, SEQ_LEN, HEAD_DIM),
            v_layer.reshape(GROUP_SIZE, ROWS_DEV, SEQ_LEN, HEAD_DIM),
        )
        context, k_upd, v_upd = lax.map(attend_block, blocks)
        attn_out = jnp.dot(context.reshape(GROUP_ROWS, ATT_WIDTH), out_weight, preferred_element_type=jnp.float32).astype(jnp.bfloat16)
        activated = jax.nn.gelu(jnp.dot(normed, up_weight, preferred_element_type=jnp.float32), approximate=False).astype(jnp.bfloat16)
        mlp_out = jnp.dot(activated, down_weight, preferred_element_type=jnp.float32)
        new_state = (hidden_state.astype(jnp.float32) + attn_out.astype(jnp.float32) + mlp_out).astype(jnp.bfloat16)
        return new_state, (k_upd.reshape(GROUP_ROWS, SEQ_LEN, HEAD_DIM), v_upd.reshape(GROUP_ROWS, SEQ_LEN, HEAD_DIM))

    final_state, new_caches = lax.scan(layer_step, hidden, (ln_gamma, ln_beta, w_qkv, w_out, w_up, w_down, k_cache, v_cache))
    return final_state, new_caches[0], new_caches[1]
```

```python
import functools

import jax
import jax.numpy as jnp
from jax import lax
from jax.experimental import pallas as pl
from jax.experimental.pallas import tpu as pltpu
from jax.sharding import PartitionSpec as P

LN_EPS = 1e-5
ROPE_BASE = 10000.0
CHUNK = 512
OUT_ROWS = 256
OUT_SLOTS = 7
F32 = jnp.float32
BF16 = jnp.bfloat16


def span(index, step, size):
    if isinstance(index, int):
        return pl.ds(index * step, size)
    return pl.ds(pl.multiple_of(index * step, step), size)


def gelu(u):
    return 0.5 * u * (1.0 + lax.erf(u * (2.0 ** -0.5)))


def mlp_kernel(layer, last, hg, x_ref, ctx_ref, gb_ref, w_up, w_down, w_out, *refs):
    if last:
        xo_ref, *refs = refs
    else:
        xo_ref, ho_ref, *refs = refs
    (wdn, hb, act, u_ref, mine, sib_send, sib_recv, sbuf, rbuf,
     w_sem, d_sem, h_sem, ss_sem, sr_sem, is_sem, ir_sem) = refs
    rows, width = x_ref.shape
    ff = w_up.shape[2]
    n_up = -(-ff // CHUNK)
    n_dn = -(-width // CHUNK)
    up_tail = ff - (n_up - 1) * CHUNK
    dn_tail = width - (n_dn - 1) * CHUNK
    size = lax.axis_size("tp")
    chips = size // 2
    me = lax.axis_index("tp")
    core = lax.rem(me, 2)
    chip = lax.div(me, 2)
    sib = 2 * chip + 1 - core
    left = 2 * lax.rem(chip + chips - 1, chips) + core
    right = 2 * lax.rem(chip + 1, chips) + core
    n_left = n_dn // 2 + 1 - core

    def up_copy(j, w):
        cols = span(j, CHUNK, w)
        return pltpu.make_async_copy(w_up.at[layer, :, cols], wup_ref().at[:, cols], w_sem.at[j])

    def dn_copy(k, w):
        cols = span(k, CHUNK, w)
        return pltpu.make_async_copy(w_down.at[layer, :, cols], wdn.at[:, cols], d_sem.at[k])

    holder = {}

    def wup_ref():
        return holder["wup"]

    def h_copies(t):
        off = jnp.where(t == 0, 2, jnp.where(t == 1, 1, jnp.where(t == 2, chips - 1, 0)))
        dest = lax.rem(chip + off, chips)
        first = pl.multiple_of((2 * dest + core) * rows, rows)
        second = pl.multiple_of((2 * dest + 1 - core) * rows, rows)
        return (
            pltpu.make_async_copy(hg.at[pl.ds(first, rows)], hb.at[pl.ds(0, rows)], h_sem.at[0]),
            pltpu.make_async_copy(hg.at[pl.ds(second, rows)], hb.at[pl.ds(rows, rows)], h_sem.at[1]),
        )

    def sib_copy(t, k):
        slot = lax.rem(t * n_dn + k, 4)
        return pltpu.make_async_remote_copy(
            src_ref=sib_send.at[slot], dst_ref=sib_recv.at[lax.rem(t, 2), k],
            send_sem=ss_sem.at[slot], recv_sem=sr_sem.at[t, k],
            device_id={"tp": sib}, device_id_type=pl.DeviceIdType.MESH)

    def ring_copy(t, k):
        goes_right = jnp.logical_or(t == 1, jnp.logical_and(t == 0, k >= n_left))
        return pltpu.make_async_remote_copy(
            src_ref=sbuf.at[t, k], dst_ref=rbuf.at[t, k],
            send_sem=is_sem.at[t, k], recv_sem=ir_sem.at[t, k],
            device_id={"tp": jnp.where(goes_right, right, left)}, device_id_type=pl.DeviceIdType.MESH)

    def up_phase(t):
        for cp in h_copies(t):
            cp.wait()

        def ready(j, w):
            @pl.when(t == 0)
            def _():
                up_copy(j, w).wait()

        def dot(j, w):
            cols = span(j, CHUNK, w)
            return jnp.dot(hb[...], wup_ref()[:, cols], preferred_element_type=F32)

        ready(0, CHUNK)
        u_ref[...] = dot(0, CHUNK)

        @pl.loop(1, n_up - 1)
        def _(j):
            ready(j, CHUNK)
            prev = span(j - 1, CHUNK, CHUNK)
            act[:, prev] = gelu(u_ref[...]).astype(BF16)
            u_ref[...] = dot(j, CHUNK)

        ready(n_up - 1, up_tail)
        act[:, (n_up - 2) * CHUNK:(n_up - 1) * CHUNK] = gelu(u_ref[...]).astype(BF16)
        act[:, (n_up - 1) * CHUNK:] = gelu(dot(n_up - 1, up_tail)).astype(BF16)

    def arrive(t, k):
        sib_copy(t, k).wait_recv()
        relay = jnp.logical_or(jnp.logical_and(t == 1, k >= n_left), jnp.logical_and(t == 2, k < n_left))

        @pl.when(relay)
        def _():
            ring_copy(0, k).wait_recv()
            mine[...] += rbuf[0, k].astype(F32)

    def settle(t, k):
        @pl.when(t == 3)
        def _():
            ring_copy(0, k).wait_send()

        sbuf[lax.rem(t, 3), k] = (mine[...] + sib_recv[lax.rem(t, 2), k].astype(F32)).astype(BF16)

    def send(t, k):
        @pl.when(t < 3)
        def _():
            ring_copy(t, k).start()

    def down_phase(t):
        def dot(k, w):
            cols = span(k, CHUNK, w)
            return jnp.dot(act[...], wdn[:, cols], preferred_element_type=F32)

        def ready(k, w):
            @pl.when(t == 0)
            def _():
                dn_copy(k, w).wait()

            @pl.when(t * n_dn + k >= 4)
            def _():
                sib_copy(t, k).wait_send()

        def place(k, w, out):
            mine[:, :w] = out[:rows]
            sib_send[lax.rem(t * n_dn + k, 4), :, :w] = out[rows:].astype(BF16)

        ready(0, CHUNK)

        @pl.when(t > 0)
        def _():
            arrive(t - 1, n_dn - 1)
            settle(t - 1, n_dn - 1)
            send(t - 1, n_dn - 1)

        place(0, CHUNK, dot(0, CHUNK))
        sib_copy(t, 0).start()

        def step(k, w):
            ready(k, w)
            arrive(t, k - 1)
            settle(t, k - 1)
            place(k, w, dot(k, w))
            send(t, k - 1)
            sib_copy(t, k).start()

        @pl.loop(1, n_dn - 1)
        def _(k):
            step(k, CHUNK)

        step(n_dn - 1, dn_tail)

    barrier = pltpu.get_barrier_semaphore()
    for other in (sib, left, right):
        pl.semaphore_signal(barrier, inc=1, device_id={"tp": other}, device_id_type=pl.DeviceIdType.MESH)

    def first_scope(wup_buf):
        holder["wup"] = wup_buf
        for cp in h_copies(0):
            cp.start()
        for j in range(n_up):
            up_copy(j, CHUNK if j < n_up - 1 else up_tail).start()
        for k in range(n_dn):
            dn_copy(k, CHUNK if k < n_dn - 1 else dn_tail).start()
        pl.semaphore_wait(barrier, 3)

        @pl.loop(0, 3)
        def _(t):
            up_phase(t)
            for cp in h_copies(t + 1):
                cp.start()
            down_phase(t)

        up_phase(3)

    pl.run_scoped(first_scope, pltpu.VMEM((width, ff), BF16))

    n_full = width // OUT_ROWS
    o_tail = width - n_full * OUT_ROWS

    def second_scope(wo, acc, xb, o_sem, x_sem):
        x_copy = pltpu.make_async_copy(x_ref, xb, x_sem)
        x_copy.start()
        def o_copy(j):
            slot = lax.rem(j, OUT_SLOTS)
            src = span(j, OUT_ROWS, OUT_ROWS)
            return pltpu.make_async_copy(w_out.at[layer, src], wo.at[slot], o_sem.at[slot])

        def tail_copy():
            slot = n_full % OUT_SLOTS
            return pltpu.make_async_copy(
                w_out.at[layer, pl.ds(n_full * OUT_ROWS, o_tail)], wo.at[slot, pl.ds(0, o_tail)], o_sem.at[slot])

        for j in range(OUT_SLOTS):
            o_copy(j).start()
        down_phase(3)
        acc[...] = jnp.zeros_like(acc)

        @pl.loop(0, n_full)
        def _(j):
            o_copy(j).wait()
            cols = span(j, OUT_ROWS, OUT_ROWS)
            acc[...] += jnp.dot(ctx_ref[:, cols], wo[lax.rem(j, OUT_SLOTS)], preferred_element_type=F32)

            @pl.when(j + OUT_SLOTS < n_full)
            def _():
                o_copy(j + OUT_SLOTS).start()

            @pl.when(j + OUT_SLOTS == n_full)
            def _():
                tail_copy().start()

        tail_copy().wait()
        acc[...] += jnp.dot(ctx_ref[:, n_full * OUT_ROWS:], wo[n_full % OUT_SLOTS, :o_tail], preferred_element_type=F32)

        arrive(3, n_dn - 1)
        settle(3, n_dn - 1)
        x_copy.wait()
        for k in range(n_dn):
            w = CHUNK if k < n_dn - 1 else dn_tail
            cols = slice(k * CHUNK, k * CHUNK + w)
            ring_copy(1, k).wait_recv()
            ring_copy(2, k).wait_recv()
            mlp = sbuf[0, k, :, :w].astype(F32) + rbuf[1, k, :, :w].astype(F32) + rbuf[2, k, :, :w].astype(F32)
            attn = acc[:, cols].astype(BF16).astype(F32)
            xo_ref[:, cols] = (xb[:, cols].astype(F32) + attn + mlp).astype(BF16)

    pl.run_scoped(
        second_scope,
        pltpu.VMEM((OUT_SLOTS, OUT_ROWS, width), BF16),
        pltpu.VMEM((rows, width), F32),
        pltpu.VMEM((rows, width), BF16),
        pltpu.SemaphoreType.DMA((OUT_SLOTS,)),
        pltpu.SemaphoreType.DMA,
    )

    if not last:
        @pl.loop(0, rows // 16)
        def _(r):
            band = pl.ds(pl.multiple_of(r * 16, 16), 16)
            values = xo_ref[band, :].astype(F32)
            centered = values - jnp.mean(values, axis=-1, keepdims=True)
            variance = jnp.mean(centered * centered, axis=-1, keepdims=True)
            ho_ref[band, :] = (centered * lax.rsqrt(variance + LN_EPS) * gb_ref[0:1, :] + gb_ref[1:2, :]).astype(BF16)

    for q in range(4):
        k = 4 * n_dn - 4 + q
        sib_copy(k // n_dn, k % n_dn).wait_send()
    for t in range(1, 3):
        for k in range(n_dn):
            ring_copy(t, k).wait_send()


def mlp_block(layer, last, hg, x, ctx, gb, w_up, w_down, w_out):
    rows, width = x.shape
    ff = w_up.shape[2]
    n_up = -(-ff // CHUNK)
    n_dn = -(-width // CHUNK)
    outs = [jax.ShapeDtypeStruct((rows, width), BF16)]
    if not last:
        outs.append(jax.ShapeDtypeStruct((rows, width), BF16))
    vmem = pl.BlockSpec(memory_space=pltpu.VMEM)
    hbm = pl.BlockSpec(memory_space=pl.ANY)
    return pl.pallas_call(
        functools.partial(mlp_kernel, layer, last),
        out_shape=outs,
        in_specs=[hbm, hbm, vmem, vmem, hbm, hbm, hbm],
        out_specs=[vmem] * len(outs),
        scratch_shapes=[
            pltpu.VMEM((ff, width), BF16),
            pltpu.VMEM((2 * rows, width), BF16),
            pltpu.VMEM((2 * rows, ff), BF16),
            pltpu.VMEM((2 * rows, CHUNK), F32),
            pltpu.VMEM((rows, CHUNK), F32),
            pltpu.VMEM((4, rows, CHUNK), BF16),
            pltpu.VMEM((2, n_dn, rows, CHUNK), BF16),
            pltpu.VMEM((3, n_dn, rows, CHUNK), BF16),
            pltpu.VMEM((3, n_dn, rows, CHUNK), BF16),
            pltpu.SemaphoreType.DMA((n_up,)),
            pltpu.SemaphoreType.DMA((n_dn,)),
            pltpu.SemaphoreType.DMA((2,)),
            pltpu.SemaphoreType.DMA((4,)),
            pltpu.SemaphoreType.DMA((4, n_dn)),
            pltpu.SemaphoreType.DMA((3, n_dn)),
            pltpu.SemaphoreType.DMA((3, n_dn)),
        ],
        compiler_params=pltpu.CompilerParams(
            collective_id=layer, has_side_effects=True, vmem_limit_bytes=67_043_328),
        cost_estimate=pl.CostEstimate(
            flops=2 * 8 * rows * width * ff * 2, bytes_accessed=130_000_000, transcendentals=8 * rows * ff),
    )(hg, x, ctx, gb, w_up, w_down, w_out)


def layer_norm(rows_in, gamma_row, beta_row):
    values = rows_in.astype(F32)
    row_mean = jnp.mean(values, axis=-1, keepdims=True)
    centered = values - row_mean
    variance = jnp.mean(centered * centered, axis=-1, keepdims=True)
    return (centered * lax.rsqrt(variance + LN_EPS) * gamma_row + beta_row).astype(BF16)


def rotary(vectors, cos_table, sin_table):
    half_dim = vectors.shape[-1] // 2
    first_half = vectors[..., :half_dim]
    second_half = vectors[..., half_dim:]
    return jnp.concatenate([first_half * cos_table - second_half * sin_table, second_half * cos_table + first_half * sin_table], axis=-1)


def local_attention(qkv_rows, positions, cos_table, sin_table, k_rows, v_rows):
    rows_n, seq_len, head_dim = k_rows.shape
    att_width = qkv_rows.shape[1] - 2 * head_dim
    num_heads = att_width // head_dim
    qkv_float = qkv_rows.astype(F32)
    query_rot = rotary(qkv_float[:, :att_width].reshape(rows_n, num_heads, head_dim), cos_table, sin_table).astype(BF16)
    key_rot = rotary(qkv_float[:, att_width:att_width + head_dim].reshape(rows_n, 1, head_dim), cos_table, sin_table).astype(BF16)
    value_new = qkv_rows[:, None, att_width + head_dim:]
    seq_ids = jnp.arange(seq_len, dtype=jnp.int32)
    write_mask = seq_ids[None, :, None] == positions[:, None, None]
    k_upd = jnp.where(write_mask, key_rot, k_rows)
    v_upd = jnp.where(write_mask, value_new, v_rows)
    scores = jnp.einsum('bhd,bsd->bhs', query_rot, k_upd, preferred_element_type=F32) * (head_dim ** -0.5)
    scores = jnp.where(seq_ids[None, None, :] <= positions[:, None, None], scores, -1e30)
    probabilities = jax.nn.softmax(scores, axis=-1).astype(BF16)
    context = jnp.einsum('bhs,bsd->bhd', probabilities, v_upd, preferred_element_type=F32)
    return context.astype(BF16).reshape(rows_n, att_width), key_rot, value_new


def device_layers(hidden, positions, ln_gamma, ln_beta, w_qkv, w_out, w_up, w_down, k_cache, v_cache):
    layers = w_qkv.shape[0]
    seq_len, head_dim = k_cache.shape[2:]
    half_dim = head_dim // 2
    inv_freq = 1.0 / (ROPE_BASE ** (jnp.arange(half_dim, dtype=F32) * (2.0 / head_dim)))
    angles = positions.astype(F32)[:, None] * inv_freq[None, :]
    cos_table = jnp.cos(angles)[:, None, :]
    sin_table = jnp.sin(angles)[:, None, :]
    x = hidden
    normed = layer_norm(x, ln_gamma[0], ln_beta[0])
    keys, values = [], []
    for layer in range(layers):
        last = layer == layers - 1
        normed_group = lax.all_gather(normed, 'tp', axis=0, tiled=True)
        qkv_rows = jnp.dot(normed, w_qkv[layer], preferred_element_type=F32).astype(BF16)
        context, key_rot, value_new = local_attention(qkv_rows, positions, cos_table, sin_table, k_cache[layer], v_cache[layer])
        keys.append(key_rot)
        values.append(value_new)
        nxt = layer if last else layer + 1
        gb = jnp.stack([ln_gamma[nxt], ln_beta[nxt]])
        outs = mlp_block(layer, last, normed_group, x, context, gb, w_up, w_down, w_out)
        x = outs[0]
        if not last:
            normed = outs[1]
    seq_ids = jnp.arange(seq_len, dtype=jnp.int32)
    mask = (seq_ids[None, :] == positions[:, None])[None, :, :, None]
    k_new = jnp.where(mask, jnp.stack(keys), k_cache)
    v_new = jnp.where(mask, jnp.stack(values), v_cache)
    return x, k_new, v_new


def solution(mesh):
    row_spec = P(('dp', 'tp'), None)
    cache_spec = P(None, ('dp', 'tp'), None, None)
    in_specs = (row_spec, P(('dp', 'tp')), P(), P(), P(), P(), P(None, None, 'tp'), P(None, 'tp', None), cache_spec, cache_spec)
    return jax.shard_map(device_layers, mesh=mesh, in_specs=in_specs, out_specs=(row_spec, cache_spec, cache_spec), check_vma=False)
```

```python
import functools

import jax
import jax.numpy as jnp
from jax import lax
from jax.experimental import pallas as pl
from jax.experimental.pallas import tpu as pltpu
from jax.sharding import PartitionSpec as P

LN_EPS = 1e-5
ROPE_BASE = 10000.0
CHUNK = 512
OUT_ROWS = 256
OUT_SLOTS = 7
F32 = jnp.float32
BF16 = jnp.bfloat16


def span(index, step, size):
    if isinstance(index, int):
        return pl.ds(index * step, size)
    return pl.ds(pl.multiple_of(index * step, step), size)


def gelu(u):
    return 0.5 * u * (1.0 + lax.erf(u * (2.0 ** -0.5)))


def mlp_kernel(layer, last, hg, x_ref, ctx_ref, gb_ref, w_up, w_down, w_out, *refs):
    if last:
        xo_ref, *refs = refs
    else:
        xo_ref, ho_ref, *refs = refs
    (wdn, hb, act, u_ref, mine, sib_send, sib_recv, sbuf, rbuf,
     w_sem, d_sem, h_sem, ss_sem, sr_sem, is_sem, ir_sem) = refs
    rows, width = x_ref.shape
    ff = w_up.shape[2]
    n_up = -(-ff // CHUNK)
    n_dn = -(-width // CHUNK)
    up_tail = ff - (n_up - 1) * CHUNK
    dn_tail = width - (n_dn - 1) * CHUNK
    size = lax.axis_size("tp")
    chips = size // 2
    me = lax.axis_index("tp")
    core = lax.rem(me, 2)
    chip = lax.div(me, 2)
    sib = 2 * chip + 1 - core
    left = 2 * lax.rem(chip + chips - 1, chips) + core
    right = 2 * lax.rem(chip + 1, chips) + core
    n_left = n_dn // 2 + 1 - core

    def up_copy(j, w):
        cols = span(j, CHUNK, w)
        return pltpu.make_async_copy(w_up.at[layer, :, cols], wup_ref().at[:, cols], w_sem.at[j])

    def dn_copy(k, w):
        cols = span(k, CHUNK, w)
        return pltpu.make_async_copy(w_down.at[layer, :, cols], wdn.at[:, cols], d_sem.at[k])

    holder = {}

    def wup_ref():
        return holder["wup"]

    def h_copies(t):
        off = jnp.where(t == 0, 2, jnp.where(t == 1, 1, jnp.where(t == 2, chips - 1, 0)))
        dest = lax.rem(chip + off, chips)
        first = pl.multiple_of((2 * dest + core) * rows, rows)
        second = pl.multiple_of((2 * dest + 1 - core) * rows, rows)
        return (
            pltpu.make_async_copy(hg.at[pl.ds(first, rows)], hb.at[pl.ds(0, rows)], h_sem.at[0]),
            pltpu.make_async_copy(hg.at[pl.ds(second, rows)], hb.at[pl.ds(rows, rows)], h_sem.at[1]),
        )

    def sib_copy(t, k):
        slot = lax.rem(t * n_dn + k, 4)
        return pltpu.make_async_remote_copy(
            src_ref=sib_send.at[slot], dst_ref=sib_recv.at[lax.rem(t, 2) * n_dn + k],
            send_sem=ss_sem.at[slot], recv_sem=sr_sem.at[t, k],
            device_id={"tp": sib}, device_id_type=pl.DeviceIdType.MESH)

    def ring_copy(t, k):
        goes_right = jnp.logical_or(t == 1, jnp.logical_and(t == 0, k >= n_left))
        return pltpu.make_async_remote_copy(
            src_ref=sbuf.at[t * n_dn + k], dst_ref=rbuf.at[t, k],
            send_sem=is_sem.at[t, k], recv_sem=ir_sem.at[t, k],
            device_id={"tp": jnp.where(goes_right, right, left)}, device_id_type=pl.DeviceIdType.MESH)

    def up_phase(t):
        for cp in h_copies(t):
            cp.wait()

        def ready(j, w):
            @pl.when(t == 0)
            def _():
                up_copy(j, w).wait()

        def dot(j, w):
            cols = span(j, CHUNK, w)
            return jnp.dot(hb[...], wup_ref()[:, cols], preferred_element_type=F32)

        ready(0, CHUNK)
        u_ref[...] = dot(0, CHUNK)

        @pl.loop(1, n_up - 1)
        def _(j):
            ready(j, CHUNK)
            prev = span(j - 1, CHUNK, CHUNK)
            act[:, prev] = gelu(u_ref[...]).astype(BF16)
            u_ref[...] = dot(j, CHUNK)

        ready(n_up - 1, up_tail)
        act[:, (n_up - 2) * CHUNK:(n_up - 1) * CHUNK] = gelu(u_ref[...]).astype(BF16)
        cols = span(n_up - 1, CHUNK, up_tail)
        for half in (pl.ds(0, rows), pl.ds(rows, rows)):
            tail = jnp.dot(hb[half, :], wup_ref()[:, cols], preferred_element_type=F32)
            act[half, (n_up - 1) * CHUNK:] = gelu(tail).astype(BF16)

    def arrive(t, k):
        sib_copy(t, k).wait_recv()
        relay = jnp.logical_or(jnp.logical_and(t == 1, k >= n_left), jnp.logical_and(t == 2, k < n_left))

        @pl.when(relay)
        def _():
            ring_copy(0, k).wait_recv()
            mine[lax.rem(t * n_dn + k, 2)] += rbuf[0, k].astype(F32)

        @pl.when(t == 3)
        def _():
            ring_copy(0, k).wait_send()

    def settle(t, k, slot, spare):
        to = jnp.where(spare, 3 * n_dn, lax.rem(t, 3) * n_dn + k)
        of = jnp.where(spare, 2 * n_dn, lax.rem(t, 2) * n_dn + k)
        sbuf[to] = (mine[slot] + sib_recv[of].astype(F32)).astype(BF16)

    def down_phase(t):
        def dot(k, w):
            return jnp.dot(act[...], wdn[:, span(k, CHUNK, w)], preferred_element_type=F32)

        def step(k, w):
            q = t * n_dn + k
            pt = jnp.maximum(jnp.where(k < 2, t - 1, t), 0)
            pk = jnp.where(k < 2, k + n_dn - 2, k - 2)
            slot = lax.rem(q, 2)

            @pl.when(t == 0)
            def _():
                dn_copy(k, w).wait()

            @pl.when(q >= 4)
            def _():
                sib_copy(t, k).wait_send()

            @pl.when(q >= 2)
            def _():
                arrive(pt, pk)

            settle(pt, pk, slot, q < 2)
            out = dot(k, w)
            mine[slot, :, :w] = out[:rows]
            sib_send[lax.rem(q, 4), :, :w] = out[rows:].astype(BF16)
            sib_copy(t, k).start()

            @pl.when(jnp.logical_and(q >= 2, pt < 3))
            def _():
                ring_copy(pt, pk).start()

        @pl.loop(0, n_dn - 1)
        def _(k):
            step(k, CHUNK)

        step(n_dn - 1, dn_tail)

    barrier = pltpu.get_barrier_semaphore()
    for other in (sib, left, right):
        pl.semaphore_signal(barrier, inc=1, device_id={"tp": other}, device_id_type=pl.DeviceIdType.MESH)

    def first_scope(wup_buf):
        holder["wup"] = wup_buf
        for cp in h_copies(0):
            cp.start()
        for j in range(n_up):
            up_copy(j, CHUNK if j < n_up - 1 else up_tail).start()
        for k in range(n_dn):
            dn_copy(k, CHUNK if k < n_dn - 1 else dn_tail).start()
        pl.semaphore_wait(barrier, 3)

        @pl.loop(0, 3)
        def _(t):
            up_phase(t)
            for cp in h_copies(t + 1):
                cp.start()
            down_phase(t)

        up_phase(3)

    pl.run_scoped(first_scope, pltpu.VMEM((width, ff), BF16))

    n_full = width // OUT_ROWS
    o_tail = width - n_full * OUT_ROWS

    def second_scope(wo, acc, xb, o_sem, x_sem):
        x_copy = pltpu.make_async_copy(x_ref, xb, x_sem)
        x_copy.start()
        def o_copy(j):
            slot = lax.rem(j, OUT_SLOTS)
            src = span(j, OUT_ROWS, OUT_ROWS)
            return pltpu.make_async_copy(w_out.at[layer, src], wo.at[slot], o_sem.at[slot])

        def tail_copy():
            slot = n_full % OUT_SLOTS
            return pltpu.make_async_copy(
                w_out.at[layer, pl.ds(n_full * OUT_ROWS, o_tail)], wo.at[slot, pl.ds(0, o_tail)], o_sem.at[slot])

        for j in range(OUT_SLOTS):
            o_copy(j).start()
        down_phase(3)
        acc[...] = jnp.zeros_like(acc)

        @pl.loop(0, n_full)
        def _(j):
            o_copy(j).wait()
            cols = span(j, OUT_ROWS, OUT_ROWS)
            acc[...] += jnp.dot(ctx_ref[:, cols], wo[lax.rem(j, OUT_SLOTS)], preferred_element_type=F32)

            @pl.when(j + OUT_SLOTS < n_full)
            def _():
                o_copy(j + OUT_SLOTS).start()

            @pl.when(j + OUT_SLOTS == n_full)
            def _():
                tail_copy().start()

        tail_copy().wait()
        acc[...] += jnp.dot(ctx_ref[:, n_full * OUT_ROWS:], wo[n_full % OUT_SLOTS, :o_tail], preferred_element_type=F32)

        for k in (n_dn - 2, n_dn - 1):
            arrive(3, k)
            settle(3, k, (3 * n_dn + k) % 2, False)
        x_copy.wait()
        for k in range(n_dn):
            w = CHUNK if k < n_dn - 1 else dn_tail
            cols = slice(k * CHUNK, k * CHUNK + w)
            ring_copy(1, k).wait_recv()
            ring_copy(2, k).wait_recv()
            mlp = sbuf[k, :, :w].astype(F32) + rbuf[1, k, :, :w].astype(F32) + rbuf[2, k, :, :w].astype(F32)
            attn = acc[:, cols].astype(BF16).astype(F32)
            xo_ref[:, cols] = (xb[:, cols].astype(F32) + attn + mlp).astype(BF16)

    pl.run_scoped(
        second_scope,
        pltpu.VMEM((OUT_SLOTS, OUT_ROWS, width), BF16),
        pltpu.VMEM((rows, width), F32),
        pltpu.VMEM((rows, width), BF16),
        pltpu.SemaphoreType.DMA((OUT_SLOTS,)),
        pltpu.SemaphoreType.DMA,
    )

    if not last:
        @pl.loop(0, rows // 16)
        def _(r):
            band = pl.ds(pl.multiple_of(r * 16, 16), 16)
            values = xo_ref[band, :].astype(F32)
            centered = values - jnp.mean(values, axis=-1, keepdims=True)
            variance = jnp.mean(centered * centered, axis=-1, keepdims=True)
            ho_ref[band, :] = (centered * lax.rsqrt(variance + LN_EPS) * gb_ref[0:1, :] + gb_ref[1:2, :]).astype(BF16)

    for q in range(4):
        k = 4 * n_dn - 4 + q
        sib_copy(k // n_dn, k % n_dn).wait_send()
    for t in range(1, 3):
        for k in range(n_dn):
            ring_copy(t, k).wait_send()


def mlp_block(layer, last, hg, x, ctx, gb, w_up, w_down, w_out):
    rows, width = x.shape
    ff = w_up.shape[2]
    n_up = -(-ff // CHUNK)
    n_dn = -(-width // CHUNK)
    outs = [jax.ShapeDtypeStruct((rows, width), BF16)]
    if not last:
        outs.append(jax.ShapeDtypeStruct((rows, width), BF16))
    vmem = pl.BlockSpec(memory_space=pltpu.VMEM)
    hbm = pl.BlockSpec(memory_space=pl.ANY)
    return pl.pallas_call(
        functools.partial(mlp_kernel, layer, last),
        out_shape=outs,
        in_specs=[hbm, hbm, vmem, vmem, hbm, hbm, hbm],
        out_specs=[vmem] * len(outs),
        scratch_shapes=[
            pltpu.VMEM((ff, width), BF16),
            pltpu.VMEM((2 * rows, width), BF16),
            pltpu.VMEM((2 * rows, ff), BF16),
            pltpu.VMEM((2 * rows, CHUNK), F32),
            pltpu.VMEM((2, rows, CHUNK), F32),
            pltpu.VMEM((4, rows, CHUNK), BF16),
            pltpu.VMEM((2 * n_dn + 1, rows, CHUNK), BF16),
            pltpu.VMEM((3 * n_dn + 1, rows, CHUNK), BF16),
            pltpu.VMEM((3, n_dn, rows, CHUNK), BF16),
            pltpu.SemaphoreType.DMA((n_up,)),
            pltpu.SemaphoreType.DMA((n_dn,)),
            pltpu.SemaphoreType.DMA((2,)),
            pltpu.SemaphoreType.DMA((4,)),
            pltpu.SemaphoreType.DMA((4, n_dn)),
            pltpu.SemaphoreType.DMA((3, n_dn)),
            pltpu.SemaphoreType.DMA((3, n_dn)),
        ],
        compiler_params=pltpu.CompilerParams(
            collective_id=layer, has_side_effects=True, vmem_limit_bytes=67_043_328),
        cost_estimate=pl.CostEstimate(
            flops=2 * 8 * rows * width * ff * 2, bytes_accessed=130_000_000, transcendentals=8 * rows * ff),
    )(hg, x, ctx, gb, w_up, w_down, w_out)


def layer_norm(rows_in, gamma_row, beta_row):
    values = rows_in.astype(F32)
    row_mean = jnp.mean(values, axis=-1, keepdims=True)
    centered = values - row_mean
    variance = jnp.mean(centered * centered, axis=-1, keepdims=True)
    return (centered * lax.rsqrt(variance + LN_EPS) * gamma_row + beta_row).astype(BF16)


def rotary(vectors, cos_table, sin_table):
    half_dim = vectors.shape[-1] // 2
    first_half = vectors[..., :half_dim]
    second_half = vectors[..., half_dim:]
    return jnp.concatenate([first_half * cos_table - second_half * sin_table, second_half * cos_table + first_half * sin_table], axis=-1)


def local_attention(qkv_rows, positions, cos_table, sin_table, k_rows, v_rows):
    rows_n, seq_len, head_dim = k_rows.shape
    att_width = qkv_rows.shape[1] - 2 * head_dim
    num_heads = att_width // head_dim
    qkv_float = qkv_rows.astype(F32)
    query_rot = rotary(qkv_float[:, :att_width].reshape(rows_n, num_heads, head_dim), cos_table, sin_table).astype(BF16)
    key_rot = rotary(qkv_float[:, att_width:att_width + head_dim].reshape(rows_n, 1, head_dim), cos_table, sin_table).astype(BF16)
    value_new = qkv_rows[:, None, att_width + head_dim:]
    seq_ids = jnp.arange(seq_len, dtype=jnp.int32)
    write_mask = seq_ids[None, :, None] == positions[:, None, None]
    k_upd = jnp.where(write_mask, key_rot, k_rows)
    v_upd = jnp.where(write_mask, value_new, v_rows)
    scores = jnp.einsum('bhd,bsd->bhs', query_rot, k_upd, preferred_element_type=F32) * (head_dim ** -0.5)
    scores = jnp.where(seq_ids[None, None, :] <= positions[:, None, None], scores, -1e30)
    probabilities = jax.nn.softmax(scores, axis=-1).astype(BF16)
    context = jnp.einsum('bhs,bsd->bhd', probabilities, v_upd, preferred_element_type=F32)
    return context.astype(BF16).reshape(rows_n, att_width), key_rot, value_new


def device_layers(hidden, positions, ln_gamma, ln_beta, w_qkv, w_out, w_up, w_down, k_cache, v_cache):
    layers = w_qkv.shape[0]
    seq_len, head_dim = k_cache.shape[2:]
    half_dim = head_dim // 2
    inv_freq = 1.0 / (ROPE_BASE ** (jnp.arange(half_dim, dtype=F32) * (2.0 / head_dim)))
    angles = positions.astype(F32)[:, None] * inv_freq[None, :]
    cos_table = jnp.cos(angles)[:, None, :]
    sin_table = jnp.sin(angles)[:, None, :]
    x = hidden
    normed = layer_norm(x, ln_gamma[0], ln_beta[0])
    keys, values = [], []
    for layer in range(layers):
        last = layer == layers - 1
        normed_group = lax.all_gather(normed, 'tp', axis=0, tiled=True)
        qkv_rows = jnp.dot(normed, w_qkv[layer], preferred_element_type=F32).astype(BF16)
        context, key_rot, value_new = local_attention(qkv_rows, positions, cos_table, sin_table, k_cache[layer], v_cache[layer])
        keys.append(key_rot)
        values.append(value_new)
        nxt = layer if last else layer + 1
        gb = jnp.stack([ln_gamma[nxt], ln_beta[nxt]])
        outs = mlp_block(layer, last, normed_group, x, context, gb, w_up, w_down, w_out)
        x = outs[0]
        if not last:
            normed = outs[1]
    seq_ids = jnp.arange(seq_len, dtype=jnp.int32)
    mask = (seq_ids[None, :] == positions[:, None])[None, :, :, None]
    k_new = jnp.where(mask, jnp.stack(keys), k_cache)
    v_new = jnp.where(mask, jnp.stack(values), v_cache)
    return x, k_new, v_new


def solution(mesh):
    row_spec = P(('dp', 'tp'), None)
    cache_spec = P(None, ('dp', 'tp'), None, None)
    in_specs = (row_spec, P(('dp', 'tp')), P(), P(), P(), P(), P(None, None, 'tp'), P(None, 'tp', None), cache_spec, cache_spec)
    return jax.shard_map(device_layers, mesh=mesh, in_specs=in_specs, out_specs=(row_spec, cache_spec, cache_spec), check_vma=False)
```

```python
import functools

import jax
import jax.numpy as jnp
from jax import lax
from jax.experimental import pallas as pl
from jax.experimental.pallas import tpu as pltpu
from jax.sharding import PartitionSpec as P

LN_EPS = 1e-5
ROPE_BASE = 10000.0
CHUNK = 512
OUT_ROWS = 256
OUT_SLOTS = 7
F32 = jnp.float32
BF16 = jnp.bfloat16


def span(index, step, size):
    if isinstance(index, int):
        return pl.ds(index * step, size)
    return pl.ds(pl.multiple_of(index * step, step), size)


def gelu(u):
    return 0.5 * u * (1.0 + lax.erf(u * (2.0 ** -0.5)))


def mlp_kernel(layer, last, hg, x_ref, ctx_ref, gb_ref, w_up, w_down, w_out, *refs):
    if last:
        xo_ref, *refs = refs
    else:
        xo_ref, ho_ref, *refs = refs
    (wdn, hb, act, u_ref, mine, sib_send, sib_recv, sbuf, rbuf,
     w_sem, d_sem, h_sem, ss_sem, sr_sem, is_sem, ir_sem) = refs
    rows, width = x_ref.shape
    ff = w_up.shape[2]
    n_up = -(-ff // CHUNK)
    n_dn = -(-width // CHUNK)
    up_tail = ff - (n_up - 1) * CHUNK
    dn_tail = width - (n_dn - 1) * CHUNK
    size = lax.axis_size("tp")
    chips = size // 2
    me = lax.axis_index("tp")
    core = lax.rem(me, 2)
    chip = lax.div(me, 2)
    sib = 2 * chip + 1 - core
    left = 2 * lax.rem(chip + chips - 1, chips) + core
    right = 2 * lax.rem(chip + 1, chips) + core
    n_left = n_dn // 2 + 1 - core

    def up_copy(j, w):
        cols = span(j, CHUNK, w)
        return pltpu.make_async_copy(w_up.at[layer, :, cols], wup_ref().at[:, cols], w_sem.at[j])

    def dn_copy(k, w):
        cols = span(k, CHUNK, w)
        return pltpu.make_async_copy(w_down.at[layer, :, cols], wdn.at[:, cols], d_sem.at[k])

    holder = {}

    def wup_ref():
        return holder["wup"]

    def h_copies(t):
        off = jnp.where(t == 0, 2, jnp.where(t == 1, 1, jnp.where(t == 2, chips - 1, 0)))
        dest = lax.rem(chip + off, chips)
        first = pl.multiple_of((2 * dest + core) * rows, rows)
        second = pl.multiple_of((2 * dest + 1 - core) * rows, rows)
        return (
            pltpu.make_async_copy(hg.at[pl.ds(first, rows)], hb.at[pl.ds(0, rows)], h_sem.at[0]),
            pltpu.make_async_copy(hg.at[pl.ds(second, rows)], hb.at[pl.ds(rows, rows)], h_sem.at[1]),
        )

    def sib_copy(t, k):
        slot = lax.rem(t * n_dn + k, 4)
        return pltpu.make_async_remote_copy(
            src_ref=sib_send.at[slot], dst_ref=sib_recv.at[lax.rem(t, 2) * n_dn + k],
            send_sem=ss_sem.at[slot], recv_sem=sr_sem.at[t, k],
            device_id={"tp": sib}, device_id_type=pl.DeviceIdType.MESH)

    def ring_copy(t, k):
        goes_right = jnp.logical_or(t == 1, jnp.logical_and(t == 0, k >= n_left))
        return pltpu.make_async_remote_copy(
            src_ref=sbuf.at[t * n_dn + k], dst_ref=rbuf.at[t, k],
            send_sem=is_sem.at[t, k], recv_sem=ir_sem.at[t, k],
            device_id={"tp": jnp.where(goes_right, right, left)}, device_id_type=pl.DeviceIdType.MESH)

    def up_phase(t):
        for cp in h_copies(t):
            cp.wait()

        def ready(j, w):
            @pl.when(t == 0)
            def _():
                up_copy(j, w).wait()

        def dot(j, w):
            cols = span(j, CHUNK, w)
            return jnp.dot(hb[...], wup_ref()[:, cols], preferred_element_type=F32)

        ready(0, CHUNK)
        u_ref[...] = dot(0, CHUNK)

        @pl.loop(1, n_up - 1)
        def _(j):
            ready(j, CHUNK)
            prev = span(j - 1, CHUNK, CHUNK)
            act[:, prev] = gelu(u_ref[...]).astype(BF16)
            u_ref[...] = dot(j, CHUNK)

        ready(n_up - 1, up_tail)
        act[:, (n_up - 2) * CHUNK:(n_up - 1) * CHUNK] = gelu(u_ref[...]).astype(BF16)
        cols = span(n_up - 1, CHUNK, up_tail)
        for half in (pl.ds(0, rows), pl.ds(rows, rows)):
            tail = jnp.dot(hb[half, :], wup_ref()[:, cols], preferred_element_type=F32)
            act[half, (n_up - 1) * CHUNK:] = gelu(tail).astype(BF16)

    def arrive(t, k):
        sib_copy(t, k).wait_recv()
        relay = jnp.logical_or(jnp.logical_and(t == 1, k >= n_left), jnp.logical_and(t == 2, k < n_left))

        @pl.when(relay)
        def _():
            ring_copy(0, k).wait_recv()
            mine[lax.rem(t * n_dn + k, 2)] += rbuf[0, k].astype(F32)

        @pl.when(t == 3)
        def _():
            ring_copy(0, k).wait_send()

    def settle(t, k, slot, spare):
        to = jnp.where(spare, 3 * n_dn, lax.rem(t, 3) * n_dn + k)
        of = jnp.where(spare, 2 * n_dn, lax.rem(t, 2) * n_dn + k)
        sbuf[to] = (mine[slot] + sib_recv[of].astype(F32)).astype(BF16)

    def down_phase(t):
        def dot(k, w):
            return jnp.dot(act[...], wdn[:, span(k, CHUNK, w)], preferred_element_type=F32)

        def step(k, w):
            q = t * n_dn + k
            pt = jnp.maximum(jnp.where(k < 2, t - 1, t), 0)
            pk = jnp.where(k < 2, k + n_dn - 2, k - 2)
            slot = lax.rem(q, 2)

            @pl.when(t == 0)
            def _():
                dn_copy(k, w).wait()

            @pl.when(q >= 4)
            def _():
                sib_copy(t, k).wait_send()

            @pl.when(q >= 2)
            def _():
                arrive(pt, pk)

            settle(pt, pk, slot, q < 2)
            out = dot(k, w)
            mine[slot, :, :w] = out[:rows]
            sib_send[lax.rem(q, 4), :, :w] = out[rows:].astype(BF16)
            sib_copy(t, k).start()

            @pl.when(jnp.logical_and(q >= 2, pt < 3))
            def _():
                ring_copy(pt, pk).start()

        @pl.loop(0, n_dn - 1)
        def _(k):
            step(k, CHUNK)

        step(n_dn - 1, dn_tail)

    barrier = pltpu.get_barrier_semaphore()
    for other in (sib, left, right):
        pl.semaphore_signal(barrier, inc=1, device_id={"tp": other}, device_id_type=pl.DeviceIdType.MESH)

    def first_scope(wup_buf):
        holder["wup"] = wup_buf
        for cp in h_copies(0):
            cp.start()
        for j in range(n_up):
            up_copy(j, CHUNK if j < n_up - 1 else up_tail).start()
        for k in range(n_dn):
            dn_copy(k, CHUNK if k < n_dn - 1 else dn_tail).start()
        pl.semaphore_wait(barrier, 3)

        @pl.loop(0, 3)
        def _(t):
            up_phase(t)
            for cp in h_copies(t + 1):
                cp.start()
            down_phase(t)

        up_phase(3)

    pl.run_scoped(first_scope, pltpu.VMEM((width, ff), BF16))

    n_full = width // OUT_ROWS
    o_tail = width - n_full * OUT_ROWS

    def second_scope(wo, acc, xb, o_sem, x_sem):
        x_copy = pltpu.make_async_copy(x_ref, xb, x_sem)
        x_copy.start()
        def o_copy(j):
            slot = lax.rem(j, OUT_SLOTS)
            src = span(j, OUT_ROWS, OUT_ROWS)
            return pltpu.make_async_copy(w_out.at[layer, src], wo.at[slot], o_sem.at[slot])

        def tail_copy():
            slot = n_full % OUT_SLOTS
            return pltpu.make_async_copy(
                w_out.at[layer, pl.ds(n_full * OUT_ROWS, o_tail)], wo.at[slot, pl.ds(0, o_tail)], o_sem.at[slot])

        for j in range(OUT_SLOTS):
            o_copy(j).start()
        down_phase(3)
        acc[...] = jnp.zeros_like(acc)

        @pl.loop(0, n_full)
        def _(j):
            o_copy(j).wait()
            cols = span(j, OUT_ROWS, OUT_ROWS)
            acc[...] += jnp.dot(ctx_ref[:, cols], wo[lax.rem(j, OUT_SLOTS)], preferred_element_type=F32)

            @pl.when(j + OUT_SLOTS < n_full)
            def _():
                o_copy(j + OUT_SLOTS).start()

            @pl.when(j + OUT_SLOTS == n_full)
            def _():
                tail_copy().start()

        tail_copy().wait()
        acc[...] += jnp.dot(ctx_ref[:, n_full * OUT_ROWS:], wo[n_full % OUT_SLOTS, :o_tail], preferred_element_type=F32)

        for k in (n_dn - 2, n_dn - 1):
            arrive(3, k)
            settle(3, k, (3 * n_dn + k) % 2, False)
        x_copy.wait()
        for k in range(n_dn):
            w = CHUNK if k < n_dn - 1 else dn_tail
            cols = slice(k * CHUNK, k * CHUNK + w)
            ring_copy(1, k).wait_recv()
            ring_copy(2, k).wait_recv()
            mlp = sbuf[k, :, :w].astype(F32) + rbuf[1, k, :, :w].astype(F32) + rbuf[2, k, :, :w].astype(F32)
            attn = acc[:, cols].astype(BF16).astype(F32)
            xo_ref[:, cols] = (xb[:, cols].astype(F32) + attn + mlp).astype(BF16)

    pl.run_scoped(
        second_scope,
        pltpu.VMEM((OUT_SLOTS, OUT_ROWS, width), BF16),
        pltpu.VMEM((rows, width), F32),
        pltpu.VMEM((rows, width), BF16),
        pltpu.SemaphoreType.DMA((OUT_SLOTS,)),
        pltpu.SemaphoreType.DMA,
    )

    if not last:
        @pl.loop(0, rows // 16)
        def _(r):
            band = pl.ds(pl.multiple_of(r * 16, 16), 16)
            values = xo_ref[band, :].astype(F32)
            centered = values - jnp.mean(values, axis=-1, keepdims=True)
            variance = jnp.mean(centered * centered, axis=-1, keepdims=True)
            ho_ref[band, :] = (centered * lax.rsqrt(variance + LN_EPS) * gb_ref[0:1, :] + gb_ref[1:2, :]).astype(BF16)

    for q in range(4):
        k = 4 * n_dn - 4 + q
        sib_copy(k // n_dn, k % n_dn).wait_send()
    for t in range(1, 3):
        for k in range(n_dn):
            ring_copy(t, k).wait_send()


def mlp_block(layer, last, hg, x, ctx, gb, w_up, w_down, w_out):
    rows, width = x.shape
    ff = w_up.shape[2]
    n_up = -(-ff // CHUNK)
    n_dn = -(-width // CHUNK)
    outs = [jax.ShapeDtypeStruct((rows, width), BF16)]
    if not last:
        outs.append(jax.ShapeDtypeStruct((rows, width), BF16))
    vmem = pl.BlockSpec(memory_space=pltpu.VMEM)
    hbm = pl.BlockSpec(memory_space=pl.ANY)
    return pl.pallas_call(
        functools.partial(mlp_kernel, layer, last),
        out_shape=outs,
        in_specs=[hbm, hbm, vmem, vmem, hbm, hbm, hbm],
        out_specs=[vmem] * len(outs),
        scratch_shapes=[
            pltpu.VMEM((ff, width), BF16),
            pltpu.VMEM((2 * rows, width), BF16),
            pltpu.VMEM((2 * rows, ff), BF16),
            pltpu.VMEM((2 * rows, CHUNK), F32),
            pltpu.VMEM((2, rows, CHUNK), F32),
            pltpu.VMEM((4, rows, CHUNK), BF16),
            pltpu.VMEM((2 * n_dn + 1, rows, CHUNK), BF16),
            pltpu.VMEM((3 * n_dn + 1, rows, CHUNK), BF16),
            pltpu.VMEM((3, n_dn, rows, CHUNK), BF16),
            pltpu.SemaphoreType.DMA((n_up,)),
            pltpu.SemaphoreType.DMA((n_dn,)),
            pltpu.SemaphoreType.DMA((2,)),
            pltpu.SemaphoreType.DMA((4,)),
            pltpu.SemaphoreType.DMA((4, n_dn)),
            pltpu.SemaphoreType.DMA((3, n_dn)),
            pltpu.SemaphoreType.DMA((3, n_dn)),
        ],
        compiler_params=pltpu.CompilerParams(
            collective_id=layer, has_side_effects=True, vmem_limit_bytes=67_043_328),
        cost_estimate=pl.CostEstimate(
            flops=2 * 8 * rows * width * ff * 2, bytes_accessed=130_000_000, transcendentals=8 * rows * ff),
    )(hg, x, ctx, gb, w_up, w_down, w_out)


def layer_norm(rows_in, gamma_row, beta_row):
    values = rows_in.astype(F32)
    row_mean = jnp.mean(values, axis=-1, keepdims=True)
    centered = values - row_mean
    variance = jnp.mean(centered * centered, axis=-1, keepdims=True)
    return (centered * lax.rsqrt(variance + LN_EPS) * gamma_row + beta_row).astype(BF16)


QKV_SLOTS = 3
ROW_BLOCK = 8
CACHE_SLOTS = 4


def attention_kernel(layer, h_ref, pos_ref, cs_ref, w_qkv, k_cache, v_cache, hg, ctx_ref, kv_ref,
                     wbuf, wtail, qp, cp, kv, kbuf, vbuf, w_sem, t_sem, kv_sem, own_sem,
                     rs_sem, rr_sem, ss_sem, sr_sem):
    rows, width = h_ref.shape
    total = w_qkv.shape[2]
    head_dim, seq_len = k_cache.shape[2:]
    stride = qp.shape[0] // rows
    n_chunks = total // CHUNK
    tail = total - n_chunks * CHUNK
    pairs = CHUNK // 128
    n_blocks = rows // ROW_BLOCK
    half = rows // 2
    scale = head_dim ** -0.5
    size = lax.axis_size("tp")
    chips = size // 2
    me = lax.axis_index("tp")
    core = lax.rem(me, 2)
    chip = lax.div(me, 2)
    sib = 2 * chip + 1 - core
    left = 2 * lax.rem(chip + chips - 1, chips) + core
    right = 2 * lax.rem(chip + 1, chips) + core
    far = 2 * lax.rem(chip + 2, chips) + core

    def part(owner, which):
        return hg.at[pl.ds(pl.multiple_of(owner * rows + which * half, half), half)]

    def whole(owner):
        return hg.at[pl.ds(pl.multiple_of(owner * rows, rows), rows)]

    def remote(src, dst, send, recv, to):
        return pltpu.make_async_remote_copy(
            src_ref=src, dst_ref=dst, send_sem=send, recv_sem=recv,
            device_id={"tp": to}, device_id_type=pl.DeviceIdType.MESH)

    def to_right(i):
        if i == 2:
            return remote(part(left, 0), part(left, 0), rs_sem.at[0, 2], rr_sem.at[0, 2], right)
        return remote(h_ref.at[pl.ds(i * half, half)], part(me, i), rs_sem.at[0, i], rr_sem.at[0, i], right)

    def to_left(i):
        if i == 2:
            return remote(part(right, 1), part(right, 1), rs_sem.at[1, 2], rr_sem.at[1, 2], left)
        return remote(h_ref.at[pl.ds((1 - i) * half, half)], part(me, 1 - i), rs_sem.at[1, i], rr_sem.at[1, i], left)

    def to_sib(i):
        block = (None, lambda: whole(left), lambda: whole(right), lambda: part(far, 0), lambda: part(far, 1))[i]
        src = h_ref if i == 0 else block()
        dst = whole(me) if i == 0 else block()
        return remote(src, dst, ss_sem.at[i], sr_sem.at[i], sib)

    own_copy = pltpu.make_async_copy(h_ref, whole(me), own_sem)

    def w_copy(j):
        cols = span(j, CHUNK, CHUNK)
        slot = j % QKV_SLOTS if isinstance(j, int) else lax.rem(j, QKV_SLOTS)
        return pltpu.make_async_copy(w_qkv.at[layer, :, cols], wbuf.at[slot], w_sem.at[slot])

    def tail_copy():
        return pltpu.make_async_copy(w_qkv.at[layer, :, pl.ds(n_chunks * CHUNK, tail)], wtail, t_sem)

    def cache_copies(i):
        slot = lax.rem(i, CACHE_SLOTS)
        at = span(i, ROW_BLOCK, ROW_BLOCK)
        return (pltpu.make_async_copy(k_cache.at[layer, at], kbuf.at[slot], kv_sem.at[0, slot]),
                pltpu.make_async_copy(v_cache.at[layer, at], vbuf.at[slot], kv_sem.at[1, slot]))

    barrier = pltpu.get_barrier_semaphore()
    for other in (sib, left, right):
        pl.semaphore_signal(barrier, inc=1, device_id={"tp": other}, device_id_type=pl.DeviceIdType.MESH)
    for j in range(QKV_SLOTS):
        w_copy(j).start()
    tail_copy().start()
    own_copy.start()
    pl.semaphore_wait(barrier, 3)
    for i in range(2):
        to_right(i).start()
        to_left(i).start()
    to_sib(0).start()

    lane = lax.broadcasted_iota(jnp.int32, (1, 128), 1)
    first = lax.rem(lane, head_dim) < head_dim // 2

    def rope(block):
        block = block.astype(BF16).astype(F32)
        ahead = pltpu.roll(block, 128 - head_dim // 2, 1)
        behind = pltpu.roll(block, head_dim // 2, 1)
        turned = block * cs_ref[0] + jnp.where(first, ahead, behind) * cs_ref[1]
        return turned.astype(BF16).astype(F32)

    def qkv_chunk(j):
        slot = j % QKV_SLOTS if isinstance(j, int) else lax.rem(j, QKV_SLOTS)
        w_copy(j).wait()
        return jnp.dot(h_ref[...], wbuf[slot], preferred_element_type=F32)

    @pl.loop(0, n_chunks - 1)
    def _(j):
        out = qkv_chunk(j)

        @pl.when(j + QKV_SLOTS < n_chunks)
        def _():
            w_copy(j + QKV_SLOTS).start()

        for i in range(pairs):
            qp[pl.ds(j * pairs + i, rows, stride), :] = rope(out[:, 128 * i:128 * (i + 1)])

    for i in range(CACHE_SLOTS):
        for cp_ in cache_copies(i):
            cp_.start()
    out = qkv_chunk(n_chunks - 1)
    turned = None
    for i in range(pairs):
        turned = rope(out[:, 128 * i:128 * (i + 1)])
        qp[pl.ds((n_chunks - 1) * pairs + i, rows, stride), :] = turned
    tail_copy().wait()
    value = jnp.dot(h_ref[...], wtail[...], preferred_element_type=F32).astype(BF16).astype(F32)
    kv[...] = jnp.concatenate([turned[:, 128 - head_dim:], value], axis=1)
    kv_ref[...] = kv[...].astype(BF16)

    slots = lax.broadcasted_iota(jnp.int32, (1, seq_len), 1)

    def attend(i):
        slot = lax.rem(i, CACHE_SLOTS)
        for cp_ in cache_copies(i):
            cp_.wait()
        queries, scores, probs = [], [], []
        for r in range(ROW_BLOCK):
            b = i * ROW_BLOCK + r
            two = qp[pl.ds(pl.multiple_of(b * stride, 8), stride), :]
            query = jnp.concatenate([two[:, :head_dim], two[:, head_dim:]], axis=0)
            queries.append(query)
            scores.append(jnp.dot(query.astype(BF16), kbuf[slot, r], preferred_element_type=F32))
        for r in range(ROW_BLOCK):
            b = i * ROW_BLOCK + r
            at = pos_ref[b]
            key = kv[pl.ds(b, 1), :head_dim]
            new = jnp.sum(queries[r] * key, axis=1, keepdims=True) * scale
            score = jnp.where(slots < at, scores[r] * scale, -1e30)
            top = jnp.maximum(jnp.max(score, axis=1, keepdims=True), new)
            weight = jnp.exp(score - top)
            new_weight = jnp.exp(new - top)
            inverse = 1.0 / (jnp.sum(weight, axis=1, keepdims=True) + new_weight)
            probs.append(((weight * inverse).astype(BF16), (new_weight * inverse).astype(BF16).astype(F32)))
        for r in range(ROW_BLOCK):
            b = i * ROW_BLOCK + r
            old, new = probs[r]
            context = lax.dot_general(old, vbuf[slot, r], (((1,), (1,)), ((), ())), preferred_element_type=F32)
            context += new * kv[pl.ds(b, 1), head_dim:]
            to = pl.ds(pl.multiple_of(b * stride, 8), stride)
            cp[to, :] = jnp.concatenate([context[:stride], context[stride:]], axis=1)

        @pl.when(i + CACHE_SLOTS < n_blocks)
        def _():
            for cp_ in cache_copies(i + CACHE_SLOTS):
                cp_.start()

    @pl.loop(0, n_blocks)
    def _(i):
        @pl.when(i == 1)
        def _():
            to_right(0).wait_recv()
            to_right(2).start()
            to_left(0).wait_recv()
            to_left(2).start()

        @pl.when(i == n_blocks - n_blocks // 4)
        def _():
            to_right(1).wait_recv()
            to_sib(1).start()
            to_left(1).wait_recv()
            to_sib(2).start()

        attend(i)

    n_pairs = -(-width // 128)
    for m in range(n_pairs):
        w = min(128, width - 128 * m)
        ctx_ref[:, 128 * m:128 * m + w] = cp[pl.ds(m, rows, stride), :][:, :w].astype(BF16)

    to_right(2).wait_recv()
    to_sib(3).start()
    to_left(2).wait_recv()
    to_sib(4).start()
    own_copy.wait()
    for i in range(3):
        to_right(i).wait_send()
        to_left(i).wait_send()
    for i in range(5):
        to_sib(i).wait()


def attention_block(layer, h, positions, cs, w_qkv, k_cache, v_cache):
    rows, width = h.shape
    head_dim, seq_len = k_cache.shape[2:]
    size = lax.axis_size("tp")
    total = w_qkv.shape[2]
    tail = total - total // CHUNK * CHUNK
    stride = -(-(-(-width // 128)) // 8) * 8
    vmem = pl.BlockSpec(memory_space=pltpu.VMEM)
    smem = pl.BlockSpec(memory_space=pltpu.SMEM)
    hbm = pl.BlockSpec(memory_space=pl.ANY)
    return pl.pallas_call(
        functools.partial(attention_kernel, layer),
        out_shape=[
            jax.ShapeDtypeStruct((size * rows, width), BF16),
            jax.ShapeDtypeStruct((rows, width), BF16),
            jax.ShapeDtypeStruct((rows, 2 * head_dim), BF16),
        ],
        in_specs=[vmem, smem, vmem, hbm, hbm, hbm],
        out_specs=[hbm, vmem, vmem],
        scratch_shapes=[
            pltpu.VMEM((QKV_SLOTS, width, CHUNK), BF16),
            pltpu.VMEM((width, tail), BF16),
            pltpu.VMEM((rows * stride, 128), F32),
            pltpu.VMEM((rows * stride, 128), F32),
            pltpu.VMEM((rows, 2 * head_dim), F32),
            pltpu.VMEM((CACHE_SLOTS, ROW_BLOCK, head_dim, seq_len), BF16),
            pltpu.VMEM((CACHE_SLOTS, ROW_BLOCK, head_dim, seq_len), BF16),
            pltpu.SemaphoreType.DMA((QKV_SLOTS,)),
            pltpu.SemaphoreType.DMA,
            pltpu.SemaphoreType.DMA((2, CACHE_SLOTS)),
            pltpu.SemaphoreType.DMA,
            pltpu.SemaphoreType.DMA((2, 3)),
            pltpu.SemaphoreType.DMA((2, 3)),
            pltpu.SemaphoreType.DMA((5,)),
            pltpu.SemaphoreType.DMA((5,)),
        ],
        compiler_params=pltpu.CompilerParams(
            collective_id=2 + layer, has_side_effects=True, vmem_limit_bytes=60_000_000),
    )(h, positions, cs, w_qkv, k_cache, v_cache)


def device_layers(hidden, positions, ln_gamma, ln_beta, w_qkv, w_out, w_up, w_down, k_cache, v_cache):
    layers = w_qkv.shape[0]
    seq_len, head_dim = k_cache.shape[2:]
    half_dim = head_dim // 2
    inv_freq = 1.0 / (ROPE_BASE ** (jnp.arange(half_dim, dtype=F32) * (2.0 / head_dim)))
    angles = positions.astype(F32)[:, None] * inv_freq[None, :]
    cos_table = jnp.cos(angles)
    sin_table = jnp.sin(angles)
    cs = jnp.stack([jnp.tile(cos_table, (1, 4)), jnp.tile(jnp.concatenate([-sin_table, sin_table], axis=1), (1, 2))])
    k_turned = jnp.swapaxes(k_cache, 2, 3)
    v_turned = jnp.swapaxes(v_cache, 2, 3)
    x = hidden
    normed = layer_norm(x, ln_gamma[0], ln_beta[0])
    rows_new = []
    for layer in range(layers):
        last = layer == layers - 1
        normed_group, context, kv = attention_block(layer, normed, positions, cs, w_qkv, k_turned, v_turned)
        rows_new.append(kv)
        nxt = layer if last else layer + 1
        gb = jnp.stack([ln_gamma[nxt], ln_beta[nxt]])
        outs = mlp_block(layer, last, normed_group, x, context, gb, w_up, w_down, w_out)
        x = outs[0]
        if not last:
            normed = outs[1]
    seq_ids = jnp.arange(seq_len, dtype=jnp.int32)
    mask = (seq_ids[None, :] == positions[:, None])[None, :, :, None]
    rows_new = jnp.stack(rows_new)[:, :, None, :]
    k_new = jnp.where(mask, rows_new[..., :head_dim], k_cache)
    v_new = jnp.where(mask, rows_new[..., head_dim:], v_cache)
    return x, k_new, v_new


def solution(mesh):
    row_spec = P(('dp', 'tp'), None)
    cache_spec = P(None, ('dp', 'tp'), None, None)
    in_specs = (row_spec, P(('dp', 'tp')), P(), P(), P(), P(), P(None, None, 'tp'), P(None, 'tp', None), cache_spec, cache_spec)
    return jax.shard_map(device_layers, mesh=mesh, in_specs=in_specs, out_specs=(row_spec, cache_spec, cache_spec), check_vma=False)
```

```python
import functools

import jax
import jax.numpy as jnp
from jax import lax
from jax.experimental import pallas as pl
from jax.experimental.pallas import tpu as pltpu
from jax.sharding import PartitionSpec as P

LN_EPS = 1e-5
ROPE_BASE = 10000.0
CHUNK = 512
QKV_SLOTS = 3
ROW_BLOCK = 8
CACHE_SLOTS = 4
F32 = jnp.float32
BF16 = jnp.bfloat16


def span(index, step, size):
    if isinstance(index, int):
        return pl.ds(index * step, size)
    return pl.ds(pl.multiple_of(index * step, step), size)


def gelu(u):
    return 0.5 * u * (1.0 + lax.erf(u * (2.0 ** -0.5)))


def layer_kernel(layer, last, h_ref, pos_ref, cs_ref, x_ref, gb_ref, w_qkv, k_cache, v_cache, w_up, w_down, w_out, *refs):
    hg, kv_ref, xo_ref, *refs = refs
    (ho_ref, wup, wtail, kv, hb, act, u_ref, mine, sib_send, sib_recv, sbuf, rbuf,
     w_sem, t_sem, kv_sem, own_sem, rs_sem, rr_sem, as_sem, ar_sem,
     u_sem, d_sem, h_sem, o_sem, x_sem, ss_sem, sr_sem, is_sem, ir_sem) = refs
    ctx_ref = ho_ref
    rows, width = h_ref.shape
    total = w_qkv.shape[2]
    head_dim, seq_len = k_cache.shape[2:]
    stride = pair_stride(width)
    n_chunks = total // CHUNK
    tail = total - n_chunks * CHUNK
    pairs = CHUNK // 128
    n_blocks = rows // ROW_BLOCK
    half = rows // 2
    scale = head_dim ** -0.5
    ff = w_up.shape[2]
    n_up = -(-ff // CHUNK)
    n_dn = -(-width // CHUNK)
    up_tail = ff - (n_up - 1) * CHUNK
    dn_tail = width - (n_dn - 1) * CHUNK
    size = lax.axis_size("tp")
    chips = size // 2
    me = lax.axis_index("tp")
    core = lax.rem(me, 2)
    chip = lax.div(me, 2)
    sib = 2 * chip + 1 - core
    left = 2 * lax.rem(chip + chips - 1, chips) + core
    right = 2 * lax.rem(chip + 1, chips) + core
    far = 2 * lax.rem(chip + 2, chips) + core
    n_left = n_dn // 2 + 1 - core

    def part(owner, which):
        return hg.at[pl.ds(pl.multiple_of(owner * rows + which * half, half), half)]

    def whole(owner):
        return hg.at[pl.ds(pl.multiple_of(owner * rows, rows), rows)]

    def remote(src, dst, send, recv, to):
        return pltpu.make_async_remote_copy(
            src_ref=src, dst_ref=dst, send_sem=send, recv_sem=recv,
            device_id={"tp": to}, device_id_type=pl.DeviceIdType.MESH)

    def to_right(i):
        if i == 2:
            return remote(part(left, 0), part(left, 0), rs_sem.at[0, 2], rr_sem.at[0, 2], right)
        return remote(h_ref.at[pl.ds(i * half, half)], part(me, i), rs_sem.at[0, i], rr_sem.at[0, i], right)

    def to_left(i):
        if i == 2:
            return remote(part(right, 1), part(right, 1), rs_sem.at[1, 2], rr_sem.at[1, 2], left)
        return remote(h_ref.at[pl.ds((1 - i) * half, half)], part(me, 1 - i), rs_sem.at[1, i], rr_sem.at[1, i], left)

    def to_sib(i):
        block = (None, lambda: whole(left), lambda: whole(right), lambda: part(far, 0), lambda: part(far, 1))[i]
        src = h_ref if i == 0 else block()
        dst = whole(me) if i == 0 else block()
        return remote(src, dst, as_sem.at[i], ar_sem.at[i], sib)

    own_copy = pltpu.make_async_copy(h_ref, whole(me), own_sem)

    def up_copy(j, w):
        cols = span(j, CHUNK, w)
        return pltpu.make_async_copy(w_up.at[layer, :, cols], wup.at[:, cols], u_sem.at[j])

    def attention_scope(wbuf, qp, kbuf, vbuf):
        def w_copy(j):
            cols = span(j, CHUNK, CHUNK)
            slot = j % QKV_SLOTS if isinstance(j, int) else lax.rem(j, QKV_SLOTS)
            return pltpu.make_async_copy(w_qkv.at[layer, :, cols], wbuf.at[slot], w_sem.at[slot])

        def qkv_tail_copy():
            return pltpu.make_async_copy(w_qkv.at[layer, :, pl.ds(n_chunks * CHUNK, tail)], wtail, t_sem)

        def cache_copies(i):
            slot = lax.rem(i, CACHE_SLOTS)
            at = span(i, ROW_BLOCK, ROW_BLOCK)
            return (pltpu.make_async_copy(k_cache.at[layer, at], kbuf.at[slot], kv_sem.at[0, slot]),
                    pltpu.make_async_copy(v_cache.at[layer, at], vbuf.at[slot], kv_sem.at[1, slot]))

        barrier = pltpu.get_barrier_semaphore()
        for other in (sib, left, right):
            pl.semaphore_signal(barrier, inc=1, device_id={"tp": other}, device_id_type=pl.DeviceIdType.MESH)
        for j in range(QKV_SLOTS):
            w_copy(j).start()
        qkv_tail_copy().start()
        own_copy.start()
        pl.semaphore_wait(barrier, 3)
        for i in range(2):
            to_right(i).start()
            to_left(i).start()
        to_sib(0).start()

        lane = lax.broadcasted_iota(jnp.int32, (1, 128), 1)
        first = lax.rem(lane, head_dim) < head_dim // 2

        def rope(block):
            block = block.astype(BF16).astype(F32)
            ahead = pltpu.roll(block, 128 - head_dim // 2, 1)
            behind = pltpu.roll(block, head_dim // 2, 1)
            turned = block * cs_ref[0] + jnp.where(first, ahead, behind) * cs_ref[1]
            return turned.astype(BF16).astype(F32)

        def qkv_chunk(j):
            slot = j % QKV_SLOTS if isinstance(j, int) else lax.rem(j, QKV_SLOTS)
            w_copy(j).wait()
            return jnp.dot(h_ref[...], wbuf[slot], preferred_element_type=F32)

        @pl.loop(0, n_chunks - 1)
        def _(j):
            out = qkv_chunk(j)

            @pl.when(j + QKV_SLOTS < n_chunks)
            def _():
                w_copy(j + QKV_SLOTS).start()

            for i in range(pairs):
                qp[pl.ds(j * pairs + i, rows, stride), :] = rope(out[:, 128 * i:128 * (i + 1)])

        for i in range(CACHE_SLOTS):
            for cp_ in cache_copies(i):
                cp_.start()
        for j in range(n_up):
            up_copy(j, CHUNK if j < n_up - 1 else up_tail).start()
        out = qkv_chunk(n_chunks - 1)
        turned = None
        for i in range(pairs):
            turned = rope(out[:, 128 * i:128 * (i + 1)])
            qp[pl.ds((n_chunks - 1) * pairs + i, rows, stride), :] = turned
        qkv_tail_copy().wait()
        value = jnp.dot(h_ref[...], wtail[...], preferred_element_type=F32).astype(BF16).astype(F32)
        kv[...] = jnp.concatenate([turned[:, 128 - head_dim:], value], axis=1)
        kv_ref[...] = kv[...].astype(BF16)

        slots = lax.broadcasted_iota(jnp.int32, (1, seq_len), 1)

        def attend(i):
            slot = lax.rem(i, CACHE_SLOTS)
            for cp_ in cache_copies(i):
                cp_.wait()
            queries, scores, probs = [], [], []
            for r in range(ROW_BLOCK):
                b = i * ROW_BLOCK + r
                two = qp[pl.ds(pl.multiple_of(b * stride, 8), stride), :]
                query = jnp.concatenate([two[:, :head_dim], two[:, head_dim:]], axis=0)
                queries.append(query)
                scores.append(jnp.dot(query.astype(BF16), kbuf[slot, r], preferred_element_type=F32))
            for r in range(ROW_BLOCK):
                b = i * ROW_BLOCK + r
                at = pos_ref[b]
                key = kv[pl.ds(b, 1), :head_dim]
                new = jnp.sum(queries[r] * key, axis=1, keepdims=True) * scale
                score = jnp.where(slots < at, scores[r] * scale, -1e30)
                top = jnp.maximum(jnp.max(score, axis=1, keepdims=True), new)
                weight = jnp.exp(score - top)
                new_weight = jnp.exp(new - top)
                inverse = 1.0 / (jnp.sum(weight, axis=1, keepdims=True) + new_weight)
                probs.append(((weight * inverse).astype(BF16), (new_weight * inverse).astype(BF16).astype(F32)))
            for r in range(ROW_BLOCK):
                b = i * ROW_BLOCK + r
                old, new = probs[r]
                context = lax.dot_general(old, vbuf[slot, r], (((1,), (1,)), ((), ())), preferred_element_type=F32)
                context += new * kv[pl.ds(b, 1), head_dim:]
                to = pl.ds(pl.multiple_of(b * stride, 8), stride)
                qp[to, :] = jnp.concatenate([context[:stride], context[stride:]], axis=1)

            @pl.when(i + CACHE_SLOTS < n_blocks)
            def _():
                for cp_ in cache_copies(i + CACHE_SLOTS):
                    cp_.start()


        @pl.loop(0, n_blocks)
        def _(i):
            @pl.when(i == 1)
            def _():
                to_right(0).wait_recv()
                to_right(2).start()
                to_left(0).wait_recv()
                to_left(2).start()

            attend(i)

        for m in range(-(-width // 128)):
            w = min(128, width - 128 * m)
            ctx_ref[:, 128 * m:128 * m + w] = qp[pl.ds(m, rows, stride), :][:, :w].astype(BF16)

    pl.run_scoped(
        attention_scope,
        pltpu.VMEM((QKV_SLOTS, width, CHUNK), BF16),
        pltpu.VMEM((rows * stride, 128), F32),
        pltpu.VMEM((CACHE_SLOTS, ROW_BLOCK, head_dim, seq_len), BF16),
        pltpu.VMEM((CACHE_SLOTS, ROW_BLOCK, head_dim, seq_len), BF16),
    )

    to_right(1).wait_recv()
    to_sib(1).start()
    to_left(1).wait_recv()
    to_sib(2).start()
    own_copy.wait()
    to_sib(0).wait_recv()

    def mlp_scope(wdn):
        def dn_copy(k, w):
            cols = span(k, CHUNK, w)
            return pltpu.make_async_copy(w_down.at[layer, :, cols], wdn.at[:, cols], d_sem.at[k])

        def h_copies(t):
            off = jnp.where(t == 0, 0, jnp.where(t == 1, 2, jnp.where(t == 2, 1, chips - 1)))
            dest = lax.rem(chip + off, chips)
            first = pl.multiple_of((2 * dest + core) * rows, rows)
            second = pl.multiple_of((2 * dest + 1 - core) * rows, rows)
            return (
                pltpu.make_async_copy(hg.at[pl.ds(first, rows)], hb.at[pl.ds(0, rows)], h_sem.at[0]),
                pltpu.make_async_copy(hg.at[pl.ds(second, rows)], hb.at[pl.ds(rows, rows)], h_sem.at[1]),
            )

        def sib_copy(t, k):
            slot = lax.rem(t * n_dn + k, 4)
            return pltpu.make_async_remote_copy(
                src_ref=sib_send.at[slot], dst_ref=sib_recv.at[lax.rem(t, 2) * n_dn + k],
                send_sem=ss_sem.at[slot], recv_sem=sr_sem.at[t, k],
                device_id={"tp": sib}, device_id_type=pl.DeviceIdType.MESH)

        def sums(t):
            return jnp.where(t == 3, 1, t)

        def ring_copy(t, k):
            goes_right = jnp.logical_or(t == 2, jnp.logical_and(t == 1, k >= n_left))
            return pltpu.make_async_remote_copy(
                src_ref=sbuf.at[sums(t) * n_dn + k], dst_ref=rbuf.at[t - 1, k],
                send_sem=is_sem.at[t - 1, k], recv_sem=ir_sem.at[t - 1, k],
                device_id={"tp": jnp.where(goes_right, right, left)}, device_id_type=pl.DeviceIdType.MESH)

        def up_phase(t):
            for cp in h_copies(t):
                cp.wait()

            def ready(j, w):
                @pl.when(t == 0)
                def _():
                    up_copy(j, w).wait()

            def dot(j, w):
                cols = span(j, CHUNK, w)
                return jnp.dot(hb[...], wup[:, cols], preferred_element_type=F32)

            ready(0, CHUNK)
            u_ref[...] = dot(0, CHUNK)

            @pl.loop(1, n_up - 1)
            def _(j):
                ready(j, CHUNK)
                prev = span(j - 1, CHUNK, CHUNK)
                act[:, prev] = gelu(u_ref[...]).astype(BF16)
                u_ref[...] = dot(j, CHUNK)

            ready(n_up - 1, up_tail)
            act[:, (n_up - 2) * CHUNK:(n_up - 1) * CHUNK] = gelu(u_ref[...]).astype(BF16)
            cols = span(n_up - 1, CHUNK, up_tail)
            for half in (pl.ds(0, rows), pl.ds(rows, rows)):
                tail = jnp.dot(hb[half, :], wup[:, cols], preferred_element_type=F32)
                act[half, (n_up - 1) * CHUNK:] = gelu(tail).astype(BF16)

        def arrive(t, k):
            sib_copy(t, k).wait_recv()
            relay = jnp.logical_or(jnp.logical_and(t == 2, k >= n_left), jnp.logical_and(t == 3, k < n_left))

            @pl.when(relay)
            def _():
                ring_copy(1, k).wait_recv()
                mine[lax.rem(t * n_dn + k, 2)] += rbuf[0, k].astype(F32)

            @pl.when(t == 3)
            def _():
                ring_copy(1, k).wait_send()

        def settle(t, k, slot, spare):
            to = jnp.where(spare, 3 * n_dn, sums(t) * n_dn + k)
            of = jnp.where(spare, 2 * n_dn, lax.rem(t, 2) * n_dn + k)
            sbuf[to] = (mine[slot] + sib_recv[of].astype(F32)).astype(BF16)

        def down_phase(t):
            def dot(k, w):
                return jnp.dot(act[...], wdn[:, span(k, CHUNK, w)], preferred_element_type=F32)

            def step(k, w):
                q = t * n_dn + k
                pt = jnp.maximum(jnp.where(k < 2, t - 1, t), 0)
                pk = jnp.where(k < 2, k + n_dn - 2, k - 2)
                slot = lax.rem(q, 2)

                @pl.when(t == 0)
                def _():
                    dn_copy(k, w).wait()

                @pl.when(q >= 4)
                def _():
                    sib_copy(t, k).wait_send()

                @pl.when(q >= 2)
                def _():
                    arrive(pt, pk)

                settle(pt, pk, slot, q < 2)
                out = dot(k, w)
                mine[slot, :, :w] = out[:rows]
                sib_send[lax.rem(q, 4), :, :w] = out[rows:].astype(BF16)
                sib_copy(t, k).start()

                @pl.when(jnp.logical_and(q >= 2, pt > 0))
                def _():
                    ring_copy(pt, pk).start()

            @pl.loop(0, n_dn - 1)
            def _(k):
                step(k, CHUNK)

            step(n_dn - 1, dn_tail)


        def out_copy(j):
            slot = j % 4 if isinstance(j, int) else lax.rem(j, 4)
            w = min(CHUNK, out_full - j * CHUNK) if isinstance(j, int) else CHUNK
            return pltpu.make_async_copy(
                w_out.at[layer, :, span(j, CHUNK, w)], wup.at[:, span(slot, CHUNK, w)], o_sem.at[slot])

        def out_chunk(j, w):
            slot = j % 4 if isinstance(j, int) else lax.rem(j, 4)
            out_copy(j).wait()
            attn = jnp.dot(ctx_ref[...], wup[:, span(slot, CHUNK, w)], preferred_element_type=F32)
            hb[:rows, span(j, CHUNK, w)] = attn.astype(BF16)

        for cp_ in h_copies(0):
            cp_.start()
        for k in range(n_dn):
            dn_copy(k, CHUNK if k < n_dn - 1 else dn_tail).start()
        @pl.loop(0, 3)
        def _(t):
            up_phase(t)

            @pl.when(t > 0)
            def _():
                for cp_ in h_copies(t + 1):
                    cp_.start()

            down_phase(t)

            @pl.when(t == 0)
            def _():
                to_right(2).wait_recv()
                to_sib(3).start()
                to_left(2).wait_recv()
                to_sib(4).start()
                for i in range(1, 5):
                    to_sib(i).wait_recv()
                for cp_ in h_copies(1):
                    cp_.start()

        up_phase(3)
        x_copy = pltpu.make_async_copy(x_ref, xo_ref, x_sem)
        x_copy.start()
        out_tail = pltpu.make_async_copy(w_out.at[layer, :, pl.ds(out_full, width - out_full)], wtail, t_sem)
        for j in range(4):
            out_copy(j).start()
        out_tail.start()
        down_phase(3)

        @pl.loop(0, n_out - 4)
        def _(j):
            out_chunk(j, CHUNK)

            @pl.when(j + 4 < n_out - 1)
            def _():
                out_copy(j + 4).start()

            @pl.when(j + 4 == n_out - 1)
            def _():
                out_copy(n_out - 1).start()

        for j in range(n_out - 4, n_out):
            out_chunk(j, min(CHUNK, out_full - j * CHUNK))
        out_tail.wait()
        hb[:rows, out_full:] = jnp.dot(ctx_ref[...], wtail[...], preferred_element_type=F32).astype(BF16)

        for k in (n_dn - 2, n_dn - 1):
            arrive(3, k)
            settle(3, k, (3 * n_dn + k) % 2, False)
            ring_copy(3, k).start()
        x_copy.wait()
        for k in range(n_dn):
            w = CHUNK if k < n_dn - 1 else dn_tail
            cols = slice(k * CHUNK, k * CHUNK + w)
            ring_copy(2, k).wait_recv()
            ring_copy(3, k).wait_recv()
            mlp = sbuf[k, :, :w].astype(F32) + rbuf[1, k, :, :w].astype(F32) + rbuf[2, k, :, :w].astype(F32)
            xo_ref[:, cols] = (xo_ref[:, cols].astype(F32) + hb[:rows, cols].astype(F32) + mlp).astype(BF16)
        for q in range(4):
            k = 4 * n_dn - 4 + q
            sib_copy(k // n_dn, k % n_dn).wait_send()
        for t in (2, 3):
            for k in range(n_dn):
                ring_copy(t, k).wait_send()

    out_full = width // 128 * 128
    n_out = -(-out_full // CHUNK)
    pl.run_scoped(mlp_scope, pltpu.VMEM((ff, width), BF16))
    for i in range(3):
        to_right(i).wait_send()
        to_left(i).wait_send()
    for i in range(5):
        to_sib(i).wait_send()

    if not last:
        @pl.loop(0, rows // 16)
        def _(r):
            band = pl.ds(pl.multiple_of(r * 16, 16), 16)
            values = xo_ref[band, :].astype(F32)
            centered = values - jnp.mean(values, axis=-1, keepdims=True)
            variance = jnp.mean(centered * centered, axis=-1, keepdims=True)
            ho_ref[band, :] = (centered * lax.rsqrt(variance + LN_EPS) * gb_ref[0:1, :] + gb_ref[1:2, :]).astype(BF16)


def pair_stride(width):
    return -(-(-(-width // 128)) // 8) * 8


def layer_block(layer, last, h, positions, cs, x, gb, w_qkv, k_cache, v_cache, w_up, w_down, w_out):
    rows, width = x.shape
    head_dim, seq_len = k_cache.shape[2:]
    ff = w_up.shape[2]
    total = w_qkv.shape[2]
    tail = total - total // CHUNK * CHUNK
    n_up = -(-ff // CHUNK)
    n_dn = -(-width // CHUNK)
    size = lax.axis_size("tp")
    vmem = pl.BlockSpec(memory_space=pltpu.VMEM)
    smem = pl.BlockSpec(memory_space=pltpu.SMEM)
    hbm = pl.BlockSpec(memory_space=pl.ANY)
    row_shape = jax.ShapeDtypeStruct((rows, width), BF16)
    outs = [
        jax.ShapeDtypeStruct((size * rows, width), BF16),
        jax.ShapeDtypeStruct((rows, 2 * head_dim), BF16),
        row_shape,
    ]
    norm_scratch = [pltpu.VMEM((rows, width), BF16)]
    if not last:
        outs.append(row_shape)
        norm_scratch = []
    return pl.pallas_call(
        functools.partial(layer_kernel, layer, last),
        out_shape=outs,
        in_specs=[vmem, smem, vmem, hbm, vmem] + [hbm] * 6,
        out_specs=[hbm] + [vmem] * (len(outs) - 1),
        scratch_shapes=norm_scratch + [
            pltpu.VMEM((width, ff), BF16),
            pltpu.VMEM((width, tail), BF16),
            pltpu.VMEM((rows, 2 * head_dim), F32),
            pltpu.VMEM((2 * rows, width), BF16),
            pltpu.VMEM((2 * rows, ff), BF16),
            pltpu.VMEM((2 * rows, CHUNK), F32),
            pltpu.VMEM((2, rows, CHUNK), F32),
            pltpu.VMEM((4, rows, CHUNK), BF16),
            pltpu.VMEM((2 * n_dn + 1, rows, CHUNK), BF16),
            pltpu.VMEM((3 * n_dn + 1, rows, CHUNK), BF16),
            pltpu.VMEM((3, n_dn, rows, CHUNK), BF16),
            pltpu.SemaphoreType.DMA((QKV_SLOTS,)),
            pltpu.SemaphoreType.DMA,
            pltpu.SemaphoreType.DMA((2, CACHE_SLOTS)),
            pltpu.SemaphoreType.DMA,
            pltpu.SemaphoreType.DMA((2, 3)),
            pltpu.SemaphoreType.DMA((2, 3)),
            pltpu.SemaphoreType.DMA((5,)),
            pltpu.SemaphoreType.DMA((5,)),
            pltpu.SemaphoreType.DMA((n_up,)),
            pltpu.SemaphoreType.DMA((n_dn,)),
            pltpu.SemaphoreType.DMA((2,)),
            pltpu.SemaphoreType.DMA((4,)),
            pltpu.SemaphoreType.DMA,
            pltpu.SemaphoreType.DMA((4,)),
            pltpu.SemaphoreType.DMA((4, n_dn)),
            pltpu.SemaphoreType.DMA((3, n_dn)),
            pltpu.SemaphoreType.DMA((3, n_dn)),
        ],
        compiler_params=pltpu.CompilerParams(
            collective_id=layer, has_side_effects=True, vmem_limit_bytes=67_043_328),
    )(h, positions, cs, x, gb, w_qkv, k_cache, v_cache, w_up, w_down, w_out)


def layer_norm(rows_in, gamma_row, beta_row):
    values = rows_in.astype(F32)
    row_mean = jnp.mean(values, axis=-1, keepdims=True)
    centered = values - row_mean
    variance = jnp.mean(centered * centered, axis=-1, keepdims=True)
    return (centered * lax.rsqrt(variance + LN_EPS) * gamma_row + beta_row).astype(BF16)


def device_layers(hidden, positions, ln_gamma, ln_beta, w_qkv, w_out, w_up, w_down, k_cache, v_cache):
    layers = w_qkv.shape[0]
    seq_len, head_dim = k_cache.shape[2:]
    half_dim = head_dim // 2
    inv_freq = 1.0 / (ROPE_BASE ** (jnp.arange(half_dim, dtype=F32) * (2.0 / head_dim)))
    angles = positions.astype(F32)[:, None] * inv_freq[None, :]
    cos_table = jnp.cos(angles)
    sin_table = jnp.sin(angles)
    cs = jnp.stack([jnp.tile(cos_table, (1, 4)), jnp.tile(jnp.concatenate([-sin_table, sin_table], axis=1), (1, 2))])
    k_turned = jnp.swapaxes(k_cache, 2, 3)
    v_turned = jnp.swapaxes(v_cache, 2, 3)
    x = hidden
    normed = layer_norm(x, ln_gamma[0], ln_beta[0])
    rows_new = []
    for layer in range(layers):
        last = layer == layers - 1
        nxt = layer if last else layer + 1
        gb = jnp.stack([ln_gamma[nxt], ln_beta[nxt]])
        outs = layer_block(layer, last, normed, positions, cs, x, gb, w_qkv, k_turned, v_turned, w_up, w_down, w_out)
        rows_new.append(outs[1])
        x = outs[2]
        if not last:
            normed = outs[3]
    seq_ids = jnp.arange(seq_len, dtype=jnp.int32)
    mask = (seq_ids[None, :] == positions[:, None])[None, :, :, None]
    rows_new = jnp.stack(rows_new)[:, :, None, :]
    k_new = jnp.where(mask, rows_new[..., :head_dim], k_cache)
    v_new = jnp.where(mask, rows_new[..., head_dim:], v_cache)
    return x, k_new, v_new


def solution(mesh):
    row_spec = P(('dp', 'tp'), None)
    cache_spec = P(None, ('dp', 'tp'), None, None)
    in_specs = (row_spec, P(('dp', 'tp')), P(), P(), P(), P(), P(None, None, 'tp'), P(None, 'tp', None), cache_spec, cache_spec)
    return jax.shard_map(device_layers, mesh=mesh, in_specs=in_specs, out_specs=(row_spec, cache_spec, cache_spec), check_vma=False)
```

```python
import functools

import jax
import jax.numpy as jnp
from jax import lax
from jax.experimental import pallas as pl
from jax.experimental.pallas import tpu as pltpu
from jax.sharding import PartitionSpec as P

LN_EPS = 1e-5
ROPE_BASE = 10000.0
CHUNK = 512
QKV_SLOTS = 3
ROW_BLOCK = 8
CACHE_SLOTS = 4
F32 = jnp.float32
BF16 = jnp.bfloat16


def span(index, step, size):
    if isinstance(index, int):
        return pl.ds(index * step, size)
    return pl.ds(pl.multiple_of(index * step, step), size)


def gelu(u):
    return 0.5 * u * (1.0 + lax.erf(u * (2.0 ** -0.5)))


def layer_kernel(layer, last, h_ref, pos_ref, cs_ref, x_ref, gb_ref, w_qkv, k_cache, v_cache, w_up, w_down, w_out, *refs):
    hg, kv_ref, xo_ref, *refs = refs
    (ho_ref, wup, wtail, kv, hb, act, u_ref, mine, sib_send, sib_recv, sbuf, rbuf,
     w_sem, t_sem, kv_sem, own_sem, rs_sem, rr_sem, as_sem, ar_sem,
     u_sem, d_sem, h_sem, o_sem, x_sem, ss_sem, sr_sem, is_sem, ir_sem) = refs
    ctx_ref = ho_ref
    rows, width = h_ref.shape
    total = w_qkv.shape[2]
    head_dim, seq_len = k_cache.shape[2:]
    stride = pair_stride(width)
    n_chunks = total // CHUNK
    tail = total - n_chunks * CHUNK
    pairs = CHUNK // 128
    n_blocks = rows // ROW_BLOCK
    half = rows // 2
    scale = head_dim ** -0.5
    ff = w_up.shape[2]
    n_up = -(-ff // CHUNK)
    n_dn = -(-width // CHUNK)
    up_tail = ff - (n_up - 1) * CHUNK
    dn_tail = width - (n_dn - 1) * CHUNK
    size = lax.axis_size("tp")
    chips = size // 2
    me = lax.axis_index("tp")
    core = lax.rem(me, 2)
    chip = lax.div(me, 2)
    sib = 2 * chip + 1 - core
    left = 2 * lax.rem(chip + chips - 1, chips) + core
    right = 2 * lax.rem(chip + 1, chips) + core
    far = 2 * lax.rem(chip + 2, chips) + core
    n_left = n_dn // 2 + 1 - core

    def part(owner, which):
        return hg.at[pl.ds(pl.multiple_of(owner * rows + which * half, half), half)]

    def whole(owner):
        return hg.at[pl.ds(pl.multiple_of(owner * rows, rows), rows)]

    def remote(src, dst, send, recv, to):
        return pltpu.make_async_remote_copy(
            src_ref=src, dst_ref=dst, send_sem=send, recv_sem=recv,
            device_id={"tp": to}, device_id_type=pl.DeviceIdType.MESH)

    def to_right(i):
        if i == 2:
            return remote(part(left, 0), part(left, 0), rs_sem.at[0, 2], rr_sem.at[0, 2], right)
        return remote(h_ref.at[pl.ds(i * half, half)], part(me, i), rs_sem.at[0, i], rr_sem.at[0, i], right)

    def to_left(i):
        if i == 2:
            return remote(part(right, 1), part(right, 1), rs_sem.at[1, 2], rr_sem.at[1, 2], left)
        return remote(h_ref.at[pl.ds((1 - i) * half, half)], part(me, 1 - i), rs_sem.at[1, i], rr_sem.at[1, i], left)

    def to_sib(i):
        block = (None, lambda: whole(left), lambda: whole(right), lambda: part(far, 0), lambda: part(far, 1))[i]
        src = h_ref if i == 0 else block()
        dst = whole(me) if i == 0 else block()
        return remote(src, dst, as_sem.at[i], ar_sem.at[i], sib)

    own_copy = pltpu.make_async_copy(h_ref, whole(me), own_sem)

    def up_copy(j, w):
        cols = span(j, CHUNK, w)
        return pltpu.make_async_copy(w_up.at[layer, :, cols], wup.at[:, cols], u_sem.at[j])

    def attention_scope(wbuf, qp, kbuf, vbuf):
        def w_copy(j):
            cols = span(j, CHUNK, CHUNK)
            slot = j % QKV_SLOTS if isinstance(j, int) else lax.rem(j, QKV_SLOTS)
            return pltpu.make_async_copy(w_qkv.at[layer, :, cols], wbuf.at[slot], w_sem.at[slot])

        def qkv_tail_copy():
            return pltpu.make_async_copy(w_qkv.at[layer, :, pl.ds(n_chunks * CHUNK, tail)], wtail, t_sem)

        def cache_copies(i):
            slot = lax.rem(i, CACHE_SLOTS)
            at = span(i, ROW_BLOCK, ROW_BLOCK)
            return (pltpu.make_async_copy(k_cache.at[layer, at], kbuf.at[slot], kv_sem.at[0, slot]),
                    pltpu.make_async_copy(v_cache.at[layer, at], vbuf.at[slot], kv_sem.at[1, slot]))

        barrier = pltpu.get_barrier_semaphore()
        for other in (sib, left, right):
            pl.semaphore_signal(barrier, inc=1, device_id={"tp": other}, device_id_type=pl.DeviceIdType.MESH)
        for j in range(QKV_SLOTS):
            w_copy(j).start()
        qkv_tail_copy().start()
        own_copy.start()
        pl.semaphore_wait(barrier, 3)
        for i in range(2):
            to_right(i).start()
            to_left(i).start()
        to_sib(0).start()

        lane = lax.broadcasted_iota(jnp.int32, (1, 128), 1)
        first = lax.rem(lane, head_dim) < head_dim // 2

        def rope(block):
            block = block.astype(BF16).astype(F32)
            ahead = pltpu.roll(block, 128 - head_dim // 2, 1)
            behind = pltpu.roll(block, head_dim // 2, 1)
            turned = block * cs_ref[0] + jnp.where(first, ahead, behind) * cs_ref[1]
            return turned.astype(BF16).astype(F32)

        def qkv_chunk(j):
            slot = j % QKV_SLOTS if isinstance(j, int) else lax.rem(j, QKV_SLOTS)
            w_copy(j).wait()
            return jnp.dot(h_ref[...], wbuf[slot], preferred_element_type=F32)

        @pl.loop(0, n_chunks - 1)
        def _(j):
            out = qkv_chunk(j)

            @pl.when(j + QKV_SLOTS < n_chunks)
            def _():
                w_copy(j + QKV_SLOTS).start()

            for i in range(pairs):
                qp[pl.ds(j * pairs + i, rows, stride), :] = rope(out[:, 128 * i:128 * (i + 1)])

        for i in range(CACHE_SLOTS):
            for cp_ in cache_copies(i):
                cp_.start()
        out = qkv_chunk(n_chunks - 1)
        turned = None
        for i in range(pairs):
            turned = rope(out[:, 128 * i:128 * (i + 1)])
            qp[pl.ds((n_chunks - 1) * pairs + i, rows, stride), :] = turned
        qkv_tail_copy().wait()
        value = jnp.dot(h_ref[...], wtail[...], preferred_element_type=F32).astype(BF16).astype(F32)
        kv[...] = jnp.concatenate([turned[:, 128 - head_dim:], value], axis=1)
        kv_ref[...] = kv[...].astype(BF16)

        slots = lax.broadcasted_iota(jnp.int32, (1, seq_len), 1)

        def attend(i):
            slot = lax.rem(i, CACHE_SLOTS)
            for cp_ in cache_copies(i):
                cp_.wait()
            queries, scores, probs = [], [], []
            for r in range(ROW_BLOCK):
                b = i * ROW_BLOCK + r
                two = qp[pl.ds(pl.multiple_of(b * stride, 8), stride), :]
                query = jnp.concatenate([two[:, :head_dim], two[:, head_dim:]], axis=0)
                queries.append(query)
                scores.append(jnp.dot(query.astype(BF16), kbuf[slot, r], preferred_element_type=F32))
            for r in range(ROW_BLOCK):
                b = i * ROW_BLOCK + r
                at = pos_ref[b]
                key = kv[pl.ds(b, 1), :head_dim]
                new = jnp.sum(queries[r] * key, axis=1, keepdims=True) * scale
                score = jnp.where(slots < at, scores[r] * scale, -1e30)
                top = jnp.maximum(jnp.max(score, axis=1, keepdims=True), new)
                weight = jnp.exp(score - top)
                new_weight = jnp.exp(new - top)
                inverse = 1.0 / (jnp.sum(weight, axis=1, keepdims=True) + new_weight)
                probs.append(((weight * inverse).astype(BF16), (new_weight * inverse).astype(BF16).astype(F32)))
            for r in range(ROW_BLOCK):
                b = i * ROW_BLOCK + r
                old, new = probs[r]
                context = lax.dot_general(old, vbuf[slot, r], (((1,), (1,)), ((), ())), preferred_element_type=F32)
                context += new * kv[pl.ds(b, 1), head_dim:]
                to = pl.ds(pl.multiple_of(b * stride, 8), stride)
                qp[to, :] = jnp.concatenate([context[:stride], context[stride:]], axis=1)

            @pl.when(i + CACHE_SLOTS < n_blocks)
            def _():
                for cp_ in cache_copies(i + CACHE_SLOTS):
                    cp_.start()


        def out_copy(j):
            slot = j % QKV_SLOTS if isinstance(j, int) else lax.rem(j, QKV_SLOTS)
            w = min(CHUNK, out_full - j * CHUNK) if isinstance(j, int) else CHUNK
            return pltpu.make_async_copy(
                w_out.at[layer, :, span(j, CHUNK, w)], wbuf.at[slot, :, pl.ds(0, w)], o_sem.at[slot])

        def out_chunk(j, w):
            slot = j % QKV_SLOTS if isinstance(j, int) else lax.rem(j, QKV_SLOTS)
            out_copy(j).wait()
            attn = jnp.dot(ctx_ref[...], wbuf[slot, :, :w], preferred_element_type=F32)
            xo_ref[:, span(j, CHUNK, w)] = attn.astype(BF16)

        out_tail = pltpu.make_async_copy(w_out.at[layer, :, pl.ds(out_full, width - out_full)], wtail, t_sem)
        for j in range(QKV_SLOTS):
            out_copy(j).start()
        out_tail.start()

        @pl.loop(0, n_blocks)
        def _(i):
            @pl.when(i == 1)
            def _():
                to_right(0).wait_recv()
                to_right(2).start()
                to_left(0).wait_recv()
                to_left(2).start()

            @pl.when(i == n_blocks // 2)
            def _():
                for j in range(n_up):
                    up_copy(j, CHUNK if j < n_up - 1 else up_tail).start()

            attend(i)

        for m in range(-(-width // 128)):
            w = min(128, width - 128 * m)
            ctx_ref[:, 128 * m:128 * m + w] = qp[pl.ds(m, rows, stride), :][:, :w].astype(BF16)

        to_right(1).wait_recv()
        to_sib(1).start()
        to_left(1).wait_recv()
        to_sib(2).start()

        @pl.loop(0, n_out - 1)
        def _(j):
            out_chunk(j, CHUNK)

            @pl.when(j + QKV_SLOTS < n_out - 1)
            def _():
                out_copy(j + QKV_SLOTS).start()

            @pl.when(j + QKV_SLOTS == n_out - 1)
            def _():
                out_copy(n_out - 1).start()

        out_chunk(n_out - 1, out_full - (n_out - 1) * CHUNK)
        out_tail.wait()
        xo_ref[:, out_full:] = jnp.dot(ctx_ref[...], wtail[...], preferred_element_type=F32).astype(BF16)

    out_full = width // 128 * 128
    n_out = -(-out_full // CHUNK)
    pl.run_scoped(
        attention_scope,
        pltpu.VMEM((QKV_SLOTS, width, CHUNK), BF16),
        pltpu.VMEM((rows * stride, 128), F32),
        pltpu.VMEM((CACHE_SLOTS, ROW_BLOCK, head_dim, seq_len), BF16),
        pltpu.VMEM((CACHE_SLOTS, ROW_BLOCK, head_dim, seq_len), BF16),
    )

    own_copy.wait()
    to_sib(0).wait_recv()

    def mlp_scope(wdn):
        def dn_copy(k, w):
            cols = span(k, CHUNK, w)
            return pltpu.make_async_copy(w_down.at[layer, :, cols], wdn.at[:, cols], d_sem.at[k])

        def h_copies(t):
            copies = []
            for i in range(4):
                own = core if i < 2 else 1 - core
                side = jnp.where(t == 0, 0, jnp.where(t == 1, 2, 1 if i % 2 == 0 else chips - 1))
                which = jnp.where(t < 2, i % 2, t - 2)
                start = (2 * lax.rem(chip + side, chips) + own) * rows + which * half
                copies.append(pltpu.make_async_copy(
                    hg.at[pl.ds(pl.multiple_of(start, half), half)], hb.at[pl.ds(i * half, half)], h_sem.at[i]))
            return copies

        def sib_copy(t, k):
            slot = lax.rem(t * n_dn + k, 4)
            return pltpu.make_async_remote_copy(
                src_ref=sib_send.at[slot], dst_ref=sib_recv.at[lax.rem(t, 2) * n_dn + k],
                send_sem=ss_sem.at[slot], recv_sem=sr_sem.at[t, k],
                device_id={"tp": sib}, device_id_type=pl.DeviceIdType.MESH)

        def sums(t):
            return jnp.where(t == 3, 1, t)

        def far_copy(k):
            return remote(sbuf.at[n_dn + k], rbuf.at[0, k], is_sem.at[0, k], ir_sem.at[0, k],
                          jnp.where(k >= n_left, right, left))

        def near_copies(t, k):
            which = t - 2
            rows_to = pl.ds(pl.multiple_of(which * half, half), half)
            return [
                remote(sbuf.at[sums(t) * n_dn + k, pl.ds(i * half, half)], rbuf.at[1 + i, k, rows_to],
                       is_sem.at[1 + 2 * i + which, k], ir_sem.at[1 + 2 * i + which, k], to)
                for i, to in enumerate((right, left))
            ]

        def up_phase(t):
            for cp in h_copies(t):
                cp.wait()

            def ready(j, w):
                @pl.when(t == 0)
                def _():
                    up_copy(j, w).wait()

            def dot(j, w):
                cols = span(j, CHUNK, w)
                return jnp.dot(hb[...], wup[:, cols], preferred_element_type=F32)

            ready(0, CHUNK)
            u_ref[...] = dot(0, CHUNK)

            @pl.loop(1, n_up - 1)
            def _(j):
                ready(j, CHUNK)
                prev = span(j - 1, CHUNK, CHUNK)
                act[:, prev] = gelu(u_ref[...]).astype(BF16)
                u_ref[...] = dot(j, CHUNK)

            ready(n_up - 1, up_tail)
            act[:, (n_up - 2) * CHUNK:(n_up - 1) * CHUNK] = gelu(u_ref[...]).astype(BF16)
            cols = span(n_up - 1, CHUNK, up_tail)
            for half in (pl.ds(0, rows), pl.ds(rows, rows)):
                tail = jnp.dot(hb[half, :], wup[:, cols], preferred_element_type=F32)
                act[half, (n_up - 1) * CHUNK:] = gelu(tail).astype(BF16)

        def arrive(t, k):
            sib_copy(t, k).wait_recv()
            @pl.when(t == 2)
            def _():
                far_copy(k).wait_recv()

            @pl.when(t >= 2)
            def _():
                on = pl.ds(pl.multiple_of(jnp.where(k >= n_left, 0, half), half), half)
                of = pl.ds(pl.multiple_of((t - 2) * half, half), half)
                mine[lax.rem(t * n_dn + k, 2), on] += rbuf[0, k, of].astype(F32)

            @pl.when(t == 3)
            def _():
                far_copy(k).wait_send()

        def settle(t, k, slot, spare):
            to = jnp.where(spare, 3 * n_dn, sums(t) * n_dn + k)
            of = jnp.where(spare, 2 * n_dn, lax.rem(t, 2) * n_dn + k)
            sbuf[to] = (mine[slot] + sib_recv[of].astype(F32)).astype(BF16)

        def down_phase(t):
            def dot(k, w):
                return jnp.dot(act[...], wdn[:, span(k, CHUNK, w)], preferred_element_type=F32)

            def step(k, w):
                q = t * n_dn + k
                pt = jnp.maximum(jnp.where(k < 2, t - 1, t), 0)
                pk = jnp.where(k < 2, k + n_dn - 2, k - 2)
                slot = lax.rem(q, 2)

                @pl.when(t == 0)
                def _():
                    dn_copy(k, w).wait()

                @pl.when(q >= 4)
                def _():
                    sib_copy(t, k).wait_send()

                @pl.when(q >= 2)
                def _():
                    arrive(pt, pk)

                settle(pt, pk, slot, q < 2)
                out = dot(k, w)
                mine[slot, :, :w] = out[:rows]
                sib_send[lax.rem(q, 4), :, :w] = out[rows:].astype(BF16)
                sib_copy(t, k).start()

                @pl.when(jnp.logical_and(q >= 2, pt == 1))
                def _():
                    far_copy(pk).start()

                @pl.when(pt >= 2)
                def _():
                    for cp_ in near_copies(pt, pk):
                        cp_.start()

            @pl.loop(0, n_dn - 1)
            def _(k):
                step(k, CHUNK)

            step(n_dn - 1, dn_tail)


        for cp_ in h_copies(0):
            cp_.start()
        for k in range(n_dn):
            dn_copy(k, CHUNK if k < n_dn - 1 else dn_tail).start()
        @pl.loop(0, 3)
        def _(t):
            up_phase(t)

            @pl.when(t > 0)
            def _():
                for cp_ in h_copies(t + 1):
                    cp_.start()

            down_phase(t)

            @pl.when(t == 0)
            def _():
                to_right(2).wait_recv()
                to_sib(3).start()
                to_left(2).wait_recv()
                to_sib(4).start()
                for i in range(1, 5):
                    to_sib(i).wait_recv()
                for cp_ in h_copies(1):
                    cp_.start()

        up_phase(3)
        x_copy = pltpu.make_async_copy(x_ref, ctx_ref, x_sem)
        x_copy.start()
        down_phase(3)

        for k in (n_dn - 2, n_dn - 1):
            arrive(3, k)
            settle(3, k, (3 * n_dn + k) % 2, False)
            for cp_ in near_copies(3, k):
                cp_.start()
        x_copy.wait()
        for k in range(n_dn):
            w = CHUNK if k < n_dn - 1 else dn_tail
            cols = slice(k * CHUNK, k * CHUNK + w)
            for cp_ in near_copies(2, k) + near_copies(3, k):
                cp_.wait_recv()
            mlp = sbuf[k, :, :w].astype(F32) + rbuf[1, k, :, :w].astype(F32) + rbuf[2, k, :, :w].astype(F32)
            xo_ref[:, cols] = (ctx_ref[:, cols].astype(F32) + xo_ref[:, cols].astype(F32) + mlp).astype(BF16)
        for q in range(4):
            k = 4 * n_dn - 4 + q
            sib_copy(k // n_dn, k % n_dn).wait_send()
        for t in (2, 3):
            for k in range(n_dn):
                for cp_ in near_copies(t, k):
                    cp_.wait_send()

    pl.run_scoped(mlp_scope, pltpu.VMEM((ff, width), BF16))
    for i in range(3):
        to_right(i).wait_send()
        to_left(i).wait_send()
    for i in range(5):
        to_sib(i).wait_send()

    if not last:
        @pl.loop(0, rows // 16)
        def _(r):
            band = pl.ds(pl.multiple_of(r * 16, 16), 16)
            values = xo_ref[band, :].astype(F32)
            centered = values - jnp.mean(values, axis=-1, keepdims=True)
            variance = jnp.mean(centered * centered, axis=-1, keepdims=True)
            ho_ref[band, :] = (centered * lax.rsqrt(variance + LN_EPS) * gb_ref[0:1, :] + gb_ref[1:2, :]).astype(BF16)


def pair_stride(width):
    return -(-(-(-width // 128)) // 8) * 8


def layer_block(layer, last, h, positions, cs, x, gb, w_qkv, k_cache, v_cache, w_up, w_down, w_out):
    rows, width = x.shape
    head_dim, seq_len = k_cache.shape[2:]
    ff = w_up.shape[2]
    total = w_qkv.shape[2]
    tail = total - total // CHUNK * CHUNK
    n_up = -(-ff // CHUNK)
    n_dn = -(-width // CHUNK)
    size = lax.axis_size("tp")
    vmem = pl.BlockSpec(memory_space=pltpu.VMEM)
    smem = pl.BlockSpec(memory_space=pltpu.SMEM)
    hbm = pl.BlockSpec(memory_space=pl.ANY)
    row_shape = jax.ShapeDtypeStruct((rows, width), BF16)
    outs = [
        jax.ShapeDtypeStruct((size * rows, width), BF16),
        jax.ShapeDtypeStruct((rows, 2 * head_dim), BF16),
        row_shape,
    ]
    norm_scratch = [pltpu.VMEM((rows, width), BF16)]
    if not last:
        outs.append(row_shape)
        norm_scratch = []
    return pl.pallas_call(
        functools.partial(layer_kernel, layer, last),
        out_shape=outs,
        in_specs=[vmem, smem, vmem, hbm, vmem] + [hbm] * 6,
        out_specs=[hbm] + [vmem] * (len(outs) - 1),
        scratch_shapes=norm_scratch + [
            pltpu.VMEM((width, ff), BF16),
            pltpu.VMEM((width, tail), BF16),
            pltpu.VMEM((rows, 2 * head_dim), F32),
            pltpu.VMEM((2 * rows, width), BF16),
            pltpu.VMEM((2 * rows, ff), BF16),
            pltpu.VMEM((2 * rows, CHUNK), F32),
            pltpu.VMEM((2, rows, CHUNK), F32),
            pltpu.VMEM((4, rows, CHUNK), BF16),
            pltpu.VMEM((2 * n_dn + 1, rows, CHUNK), BF16),
            pltpu.VMEM((3 * n_dn + 1, rows, CHUNK), BF16),
            pltpu.VMEM((3, n_dn, rows, CHUNK), BF16),
            pltpu.SemaphoreType.DMA((QKV_SLOTS,)),
            pltpu.SemaphoreType.DMA,
            pltpu.SemaphoreType.DMA((2, CACHE_SLOTS)),
            pltpu.SemaphoreType.DMA,
            pltpu.SemaphoreType.DMA((2, 3)),
            pltpu.SemaphoreType.DMA((2, 3)),
            pltpu.SemaphoreType.DMA((5,)),
            pltpu.SemaphoreType.DMA((5,)),
            pltpu.SemaphoreType.DMA((n_up,)),
            pltpu.SemaphoreType.DMA((n_dn,)),
            pltpu.SemaphoreType.DMA((4,)),
            pltpu.SemaphoreType.DMA((QKV_SLOTS,)),
            pltpu.SemaphoreType.DMA,
            pltpu.SemaphoreType.DMA((4,)),
            pltpu.SemaphoreType.DMA((4, n_dn)),
            pltpu.SemaphoreType.DMA((5, n_dn)),
            pltpu.SemaphoreType.DMA((5, n_dn)),
        ],
        compiler_params=pltpu.CompilerParams(
            collective_id=layer, has_side_effects=True, vmem_limit_bytes=67_043_328),
    )(h, positions, cs, x, gb, w_qkv, k_cache, v_cache, w_up, w_down, w_out)


def layer_norm(rows_in, gamma_row, beta_row):
    values = rows_in.astype(F32)
    row_mean = jnp.mean(values, axis=-1, keepdims=True)
    centered = values - row_mean
    variance = jnp.mean(centered * centered, axis=-1, keepdims=True)
    return (centered * lax.rsqrt(variance + LN_EPS) * gamma_row + beta_row).astype(BF16)


def device_layers(hidden, positions, ln_gamma, ln_beta, w_qkv, w_out, w_up, w_down, k_cache, v_cache):
    layers = w_qkv.shape[0]
    seq_len, head_dim = k_cache.shape[2:]
    half_dim = head_dim // 2
    inv_freq = 1.0 / (ROPE_BASE ** (jnp.arange(half_dim, dtype=F32) * (2.0 / head_dim)))
    angles = positions.astype(F32)[:, None] * inv_freq[None, :]
    cos_table = jnp.cos(angles)
    sin_table = jnp.sin(angles)
    cs = jnp.stack([jnp.tile(cos_table, (1, 4)), jnp.tile(jnp.concatenate([-sin_table, sin_table], axis=1), (1, 2))])
    k_turned = jnp.swapaxes(k_cache, 2, 3)
    v_turned = jnp.swapaxes(v_cache, 2, 3)
    x = hidden
    normed = layer_norm(x, ln_gamma[0], ln_beta[0])
    rows_new = []
    for layer in range(layers):
        last = layer == layers - 1
        nxt = layer if last else layer + 1
        gb = jnp.stack([ln_gamma[nxt], ln_beta[nxt]])
        outs = layer_block(layer, last, normed, positions, cs, x, gb, w_qkv, k_turned, v_turned, w_up, w_down, w_out)
        rows_new.append(outs[1])
        x = outs[2]
        if not last:
            normed = outs[3]
    seq_ids = jnp.arange(seq_len, dtype=jnp.int32)
    mask = (seq_ids[None, :] == positions[:, None])[None, :, :, None]
    rows_new = jnp.stack(rows_new)[:, :, None, :]
    k_new = jnp.where(mask, rows_new[..., :head_dim], k_cache)
    v_new = jnp.where(mask, rows_new[..., head_dim:], v_cache)
    return x, k_new, v_new


def solution(mesh):
    row_spec = P(('dp', 'tp'), None)
    cache_spec = P(None, ('dp', 'tp'), None, None)
    in_specs = (row_spec, P(('dp', 'tp')), P(), P(), P(), P(), P(None, None, 'tp'), P(None, 'tp', None), cache_spec, cache_spec)
    return jax.shard_map(device_layers, mesh=mesh, in_specs=in_specs, out_specs=(row_spec, cache_spec, cache_spec), check_vma=False)
```

```python
import functools

import jax
import jax.numpy as jnp
from jax import lax
from jax.experimental import pallas as pl
from jax.experimental.pallas import tpu as pltpu
from jax.sharding import PartitionSpec as P

LN_EPS = 1e-5
ROPE_BASE = 10000.0
CHUNK = 512
QKV_SLOTS = 3
ROW_BLOCK = 8
CACHE_SLOTS = 4
F32 = jnp.float32
BF16 = jnp.bfloat16


def span(index, step, size):
    if isinstance(index, int):
        return pl.ds(index * step, size)
    return pl.ds(pl.multiple_of(index * step, step), size)


def gelu(u):
    return 0.5 * u * (1.0 + lax.erf(u * (2.0 ** -0.5)))


def layer_kernel(layer, last, h_ref, pos_ref, cs_ref, x_ref, gb_ref, w_qkv, k_cache, v_cache, w_up, w_down, w_out, *refs):
    hg, kv_ref, xo_ref, *refs = refs
    (ho_ref, wup, wtail, kv, hb, act, u_ref, mine, sib_send, sib_recv, sbuf, rbuf,
     w_sem, t_sem, kv_sem, own_sem, rs_sem, rr_sem, as_sem, ar_sem,
     u_sem, d_sem, h_sem, o_sem, x_sem, ss_sem, sr_sem, is_sem, ir_sem) = refs
    ctx_ref = ho_ref
    rows, width = h_ref.shape
    total = w_qkv.shape[2]
    head_dim, seq_len = k_cache.shape[2:]
    stride = pair_stride(width)
    n_chunks = total // CHUNK
    tail = total - n_chunks * CHUNK
    pairs = CHUNK // 128
    n_blocks = rows // ROW_BLOCK
    half = rows // 2
    scale = head_dim ** -0.5
    ff = w_up.shape[2]
    n_up = -(-ff // CHUNK)
    n_dn = -(-width // CHUNK)
    up_tail = ff - (n_up - 1) * CHUNK
    dn_tail = width - (n_dn - 1) * CHUNK
    size = lax.axis_size("tp")
    chips = size // 2
    me = lax.axis_index("tp")
    core = lax.rem(me, 2)
    chip = lax.div(me, 2)
    sib = 2 * chip + 1 - core
    left = 2 * lax.rem(chip + chips - 1, chips) + core
    right = 2 * lax.rem(chip + 1, chips) + core
    far = 2 * lax.rem(chip + 2, chips) + core
    n_left = n_dn // 2 + 1 - core

    def part(owner, which):
        return hg.at[pl.ds(pl.multiple_of(owner * rows + which * half, half), half)]

    def whole(owner):
        return hg.at[pl.ds(pl.multiple_of(owner * rows, rows), rows)]

    def remote(src, dst, send, recv, to):
        return pltpu.make_async_remote_copy(
            src_ref=src, dst_ref=dst, send_sem=send, recv_sem=recv,
            device_id={"tp": to}, device_id_type=pl.DeviceIdType.MESH)

    def to_right(i):
        if i == 2:
            return remote(part(left, 0), part(left, 0), rs_sem.at[0, 2], rr_sem.at[0, 2], right)
        return remote(h_ref.at[pl.ds(i * half, half)], part(me, i), rs_sem.at[0, i], rr_sem.at[0, i], right)

    def to_left(i):
        if i == 2:
            return remote(part(right, 1), part(right, 1), rs_sem.at[1, 2], rr_sem.at[1, 2], left)
        return remote(h_ref.at[pl.ds((1 - i) * half, half)], part(me, 1 - i), rs_sem.at[1, i], rr_sem.at[1, i], left)

    def to_sib(i):
        block = (None, lambda: whole(left), lambda: whole(right), lambda: part(far, 0), lambda: part(far, 1))[i]
        src = h_ref if i == 0 else block()
        dst = whole(me) if i == 0 else block()
        return remote(src, dst, as_sem.at[i], ar_sem.at[i], sib)

    own_copy = pltpu.make_async_copy(h_ref, whole(me), own_sem)

    def up_copy(j, w):
        cols = span(j, CHUNK, w)
        return pltpu.make_async_copy(w_up.at[layer, :, cols], wup.at[:, cols], u_sem.at[j])

    def attention_scope(wbuf, qp, kbuf, vbuf):
        def w_copy(j):
            cols = span(j, CHUNK, CHUNK)
            slot = j % QKV_SLOTS if isinstance(j, int) else lax.rem(j, QKV_SLOTS)
            return pltpu.make_async_copy(w_qkv.at[layer, :, cols], wbuf.at[slot], w_sem.at[slot])

        def qkv_tail_copy():
            return pltpu.make_async_copy(w_qkv.at[layer, :, pl.ds(n_chunks * CHUNK, tail)], wtail, t_sem)

        def cache_copies(i):
            slot = lax.rem(i, CACHE_SLOTS)
            at = span(i, ROW_BLOCK, ROW_BLOCK)
            return (pltpu.make_async_copy(k_cache.at[layer, at], kbuf.at[slot], kv_sem.at[0, slot]),
                    pltpu.make_async_copy(v_cache.at[layer, at], vbuf.at[slot], kv_sem.at[1, slot]))

        barrier = pltpu.get_barrier_semaphore()
        for other in (sib, left, right):
            pl.semaphore_signal(barrier, inc=1, device_id={"tp": other}, device_id_type=pl.DeviceIdType.MESH)
        for j in range(QKV_SLOTS):
            w_copy(j).start()
        qkv_tail_copy().start()
        own_copy.start()
        pl.semaphore_wait(barrier, 3)
        for i in range(2):
            to_right(i).start()
            to_left(i).start()
        to_sib(0).start()

        lane = lax.broadcasted_iota(jnp.int32, (1, 128), 1)
        first = lax.rem(lane, head_dim) < head_dim // 2

        def rope(block):
            block = block.astype(BF16).astype(F32)
            ahead = pltpu.roll(block, 128 - head_dim // 2, 1)
            behind = pltpu.roll(block, head_dim // 2, 1)
            turned = block * cs_ref[0] + jnp.where(first, ahead, behind) * cs_ref[1]
            return turned.astype(BF16).astype(F32)

        def qkv_chunk(j):
            slot = j % QKV_SLOTS if isinstance(j, int) else lax.rem(j, QKV_SLOTS)
            w_copy(j).wait()
            return jnp.dot(h_ref[...], wbuf[slot], preferred_element_type=F32)

        @pl.loop(0, n_chunks - 1)
        def _(j):
            out = qkv_chunk(j)

            @pl.when(j + QKV_SLOTS < n_chunks)
            def _():
                w_copy(j + QKV_SLOTS).start()

            for i in range(pairs):
                qp[pl.ds(j * pairs + i, rows, stride), :] = rope(out[:, 128 * i:128 * (i + 1)])

        for i in range(CACHE_SLOTS):
            for cp_ in cache_copies(i):
                cp_.start()
        for j in range(n_up):
            up_copy(j, CHUNK if j < n_up - 1 else up_tail).start()
        out = qkv_chunk(n_chunks - 1)
        turned = None
        for i in range(pairs):
            turned = rope(out[:, 128 * i:128 * (i + 1)])
            qp[pl.ds((n_chunks - 1) * pairs + i, rows, stride), :] = turned
        qkv_tail_copy().wait()
        value = jnp.dot(h_ref[...], wtail[...], preferred_element_type=F32).astype(BF16).astype(F32)
        kv[...] = jnp.concatenate([turned[:, 128 - head_dim:], value], axis=1)
        kv_ref[...] = kv[...].astype(BF16)

        slots = lax.broadcasted_iota(jnp.int32, (1, seq_len), 1)

        def attend(i):
            slot = lax.rem(i, CACHE_SLOTS)
            for cp_ in cache_copies(i):
                cp_.wait()
            queries, scores, probs = [], [], []
            for r in range(ROW_BLOCK):
                b = i * ROW_BLOCK + r
                two = qp[pl.ds(pl.multiple_of(b * stride, 8), stride), :]
                query = jnp.concatenate([two[:, :head_dim], two[:, head_dim:]], axis=0)
                queries.append(query)
                scores.append(jnp.dot(query.astype(BF16), kbuf[slot, r], preferred_element_type=F32))
            for r in range(ROW_BLOCK):
                b = i * ROW_BLOCK + r
                at = pos_ref[b]
                key = kv[pl.ds(b, 1), :head_dim]
                new = jnp.sum(queries[r] * key, axis=1, keepdims=True) * scale
                score = jnp.where(slots < at, scores[r] * scale, -1e30)
                top = jnp.maximum(jnp.max(score, axis=1, keepdims=True), new)
                weight = jnp.exp(score - top)
                new_weight = jnp.exp(new - top)
                inverse = 1.0 / (jnp.sum(weight, axis=1, keepdims=True) + new_weight)
                probs.append(((weight * inverse).astype(BF16), (new_weight * inverse).astype(BF16).astype(F32)))
            for r in range(ROW_BLOCK):
                b = i * ROW_BLOCK + r
                old, new = probs[r]
                context = lax.dot_general(old, vbuf[slot, r], (((1,), (1,)), ((), ())), preferred_element_type=F32)
                context += new * kv[pl.ds(b, 1), head_dim:]
                to = pl.ds(pl.multiple_of(b * stride, 8), stride)
                qp[to, :] = jnp.concatenate([context[:stride], context[stride:]], axis=1)

            @pl.when(i + CACHE_SLOTS < n_blocks)
            def _():
                for cp_ in cache_copies(i + CACHE_SLOTS):
                    cp_.start()


        @pl.loop(0, n_blocks)
        def _(i):
            @pl.when(i == 1)
            def _():
                to_right(0).wait_recv()
                to_right(2).start()
                to_left(0).wait_recv()
                to_left(2).start()

            attend(i)

        for m in range(-(-width // 128)):
            w = min(128, width - 128 * m)
            ctx_ref[:, 128 * m:128 * m + w] = qp[pl.ds(m, rows, stride), :][:, :w].astype(BF16)

    pl.run_scoped(
        attention_scope,
        pltpu.VMEM((QKV_SLOTS, width, CHUNK), BF16),
        pltpu.VMEM((rows * stride, 128), F32),
        pltpu.VMEM((CACHE_SLOTS, ROW_BLOCK, head_dim, seq_len), BF16),
        pltpu.VMEM((CACHE_SLOTS, ROW_BLOCK, head_dim, seq_len), BF16),
    )

    to_right(1).wait_recv()
    to_sib(1).start()
    to_left(1).wait_recv()
    to_sib(2).start()
    own_copy.wait()
    to_sib(0).wait_recv()

    def mlp_scope(wdn):
        def dn_copy(k, w):
            cols = span(k, CHUNK, w)
            return pltpu.make_async_copy(w_down.at[layer, :, cols], wdn.at[:, cols], d_sem.at[k])

        def h_copies(t):
            copies = []
            for i in range(4):
                own = core if i < 2 else 1 - core
                side = jnp.where(t == 0, 0, jnp.where(t == 1, 2, 1 if i % 2 == 0 else chips - 1))
                which = jnp.where(t < 2, i % 2, t - 2)
                start = (2 * lax.rem(chip + side, chips) + own) * rows + which * half
                copies.append(pltpu.make_async_copy(
                    hg.at[pl.ds(pl.multiple_of(start, half), half)], hb.at[pl.ds(i * half, half)], h_sem.at[i]))
            return copies

        def sib_copy(t, k):
            slot = lax.rem(t * n_dn + k, 4)
            return pltpu.make_async_remote_copy(
                src_ref=sib_send.at[slot], dst_ref=sib_recv.at[lax.rem(t, 2) * n_dn + k],
                send_sem=ss_sem.at[slot], recv_sem=sr_sem.at[t, k],
                device_id={"tp": sib}, device_id_type=pl.DeviceIdType.MESH)

        def sums(t):
            return jnp.where(t == 3, 1, t)

        def far_copy(k):
            return remote(sbuf.at[n_dn + k], rbuf.at[0, k], is_sem.at[0, k], ir_sem.at[0, k],
                          jnp.where(k >= n_left, right, left))

        def near_copies(t, k):
            which = t - 2
            rows_to = pl.ds(pl.multiple_of(which * half, half), half)
            return [
                remote(sbuf.at[sums(t) * n_dn + k, pl.ds(i * half, half)], rbuf.at[1 + i, k, rows_to],
                       is_sem.at[1 + 2 * i + which, k], ir_sem.at[1 + 2 * i + which, k], to)
                for i, to in enumerate((right, left))
            ]

        def up_phase(t):
            for cp in h_copies(t):
                cp.wait()

            def ready(j, w):
                @pl.when(t == 0)
                def _():
                    up_copy(j, w).wait()

            def dot(j, w):
                cols = span(j, CHUNK, w)
                return jnp.dot(hb[...], wup[:, cols], preferred_element_type=F32)

            ready(0, CHUNK)
            u_ref[...] = dot(0, CHUNK)

            @pl.loop(1, n_up - 1)
            def _(j):
                ready(j, CHUNK)
                prev = span(j - 1, CHUNK, CHUNK)
                act[:, prev] = gelu(u_ref[...]).astype(BF16)
                u_ref[...] = dot(j, CHUNK)

            ready(n_up - 1, up_tail)
            act[:, (n_up - 2) * CHUNK:(n_up - 1) * CHUNK] = gelu(u_ref[...]).astype(BF16)
            cols = span(n_up - 1, CHUNK, up_tail)
            for half in (pl.ds(0, rows), pl.ds(rows, rows)):
                tail = jnp.dot(hb[half, :], wup[:, cols], preferred_element_type=F32)
                act[half, (n_up - 1) * CHUNK:] = gelu(tail).astype(BF16)

        def arrive(t, k):
            sib_copy(t, k).wait_recv()
            @pl.when(t == 2)
            def _():
                far_copy(k).wait_recv()

            @pl.when(t >= 2)
            def _():
                on = pl.ds(pl.multiple_of(jnp.where(k >= n_left, 0, half), half), half)
                of = pl.ds(pl.multiple_of((t - 2) * half, half), half)
                mine[lax.rem(t * n_dn + k, 2), on] += rbuf[0, k, of].astype(F32)

            @pl.when(t == 3)
            def _():
                far_copy(k).wait_send()

        def settle(t, k, slot, spare):
            to = jnp.where(spare, 3 * n_dn, sums(t) * n_dn + k)
            of = jnp.where(spare, 2 * n_dn, lax.rem(t, 2) * n_dn + k)
            sbuf[to] = (mine[slot] + sib_recv[of].astype(F32)).astype(BF16)

        def down_phase(t):
            def dot(k, w):
                return jnp.dot(act[...], wdn[:, span(k, CHUNK, w)], preferred_element_type=F32)

            def step(k, w):
                q = t * n_dn + k
                pt = jnp.maximum(jnp.where(k < 2, t - 1, t), 0)
                pk = jnp.where(k < 2, k + n_dn - 2, k - 2)
                slot = lax.rem(q, 2)

                @pl.when(t == 0)
                def _():
                    dn_copy(k, w).wait()

                @pl.when(q >= 4)
                def _():
                    sib_copy(t, k).wait_send()

                @pl.when(q >= 2)
                def _():
                    arrive(pt, pk)

                settle(pt, pk, slot, q < 2)
                out = dot(k, w)
                mine[slot, :, :w] = out[:rows]
                sib_send[lax.rem(q, 4), :, :w] = out[rows:].astype(BF16)
                sib_copy(t, k).start()

                @pl.when(jnp.logical_and(q >= 2, pt == 1))
                def _():
                    far_copy(pk).start()

                @pl.when(pt >= 2)
                def _():
                    for cp_ in near_copies(pt, pk):
                        cp_.start()

            @pl.loop(0, n_dn - 1)
            def _(k):
                step(k, CHUNK)

            step(n_dn - 1, dn_tail)


        def out_copy(j):
            slot = j % 4 if isinstance(j, int) else lax.rem(j, 4)
            w = min(CHUNK, out_full - j * CHUNK) if isinstance(j, int) else CHUNK
            return pltpu.make_async_copy(
                w_out.at[layer, :, span(j, CHUNK, w)], wup.at[:, span(slot, CHUNK, w)], o_sem.at[slot])

        def out_chunk(j, w):
            slot = j % 4 if isinstance(j, int) else lax.rem(j, 4)
            out_copy(j).wait()
            attn = jnp.dot(ctx_ref[...], wup[:, span(slot, CHUNK, w)], preferred_element_type=F32)
            hb[:rows, span(j, CHUNK, w)] = attn.astype(BF16)

        for cp_ in h_copies(0):
            cp_.start()
        for k in range(n_dn):
            dn_copy(k, CHUNK if k < n_dn - 1 else dn_tail).start()
        @pl.loop(0, 3)
        def _(t):
            up_phase(t)

            @pl.when(t > 0)
            def _():
                for cp_ in h_copies(t + 1):
                    cp_.start()

            down_phase(t)

            @pl.when(t == 0)
            def _():
                to_right(2).wait_recv()
                to_sib(3).start()
                to_left(2).wait_recv()
                to_sib(4).start()
                for i in range(1, 5):
                    to_sib(i).wait_recv()
                for cp_ in h_copies(1):
                    cp_.start()

        up_phase(3)
        x_copy = pltpu.make_async_copy(x_ref, xo_ref, x_sem)
        x_copy.start()
        out_tail = pltpu.make_async_copy(w_out.at[layer, :, pl.ds(out_full, width - out_full)], wtail, t_sem)
        for j in range(4):
            out_copy(j).start()
        out_tail.start()
        down_phase(3)

        @pl.loop(0, n_out - 4)
        def _(j):
            out_chunk(j, CHUNK)

            @pl.when(j + 4 < n_out - 1)
            def _():
                out_copy(j + 4).start()

            @pl.when(j + 4 == n_out - 1)
            def _():
                out_copy(n_out - 1).start()

        for j in range(n_out - 4, n_out):
            out_chunk(j, min(CHUNK, out_full - j * CHUNK))
        out_tail.wait()
        hb[:rows, out_full:] = jnp.dot(ctx_ref[...], wtail[...], preferred_element_type=F32).astype(BF16)

        for k in (n_dn - 2, n_dn - 1):
            arrive(3, k)
            settle(3, k, (3 * n_dn + k) % 2, False)
            for cp_ in near_copies(3, k):
                cp_.start()
        x_copy.wait()
        for k in range(n_dn):
            w = CHUNK if k < n_dn - 1 else dn_tail
            cols = slice(k * CHUNK, k * CHUNK + w)
            for cp_ in near_copies(2, k) + near_copies(3, k):
                cp_.wait_recv()
            mlp = sbuf[k, :, :w].astype(F32) + rbuf[1, k, :, :w].astype(F32) + rbuf[2, k, :, :w].astype(F32)
            xo_ref[:, cols] = (xo_ref[:, cols].astype(F32) + hb[:rows, cols].astype(F32) + mlp).astype(BF16)
        for q in range(4):
            k = 4 * n_dn - 4 + q
            sib_copy(k // n_dn, k % n_dn).wait_send()
        for t in (2, 3):
            for k in range(n_dn):
                for cp_ in near_copies(t, k):
                    cp_.wait_send()

    out_full = width // 128 * 128
    n_out = -(-out_full // CHUNK)
    pl.run_scoped(mlp_scope, pltpu.VMEM((ff, width), BF16))
    for i in range(3):
        to_right(i).wait_send()
        to_left(i).wait_send()
    for i in range(5):
        to_sib(i).wait_send()

    if not last:
        @pl.loop(0, rows // 16)
        def _(r):
            band = pl.ds(pl.multiple_of(r * 16, 16), 16)
            values = xo_ref[band, :].astype(F32)
            centered = values - jnp.mean(values, axis=-1, keepdims=True)
            variance = jnp.mean(centered * centered, axis=-1, keepdims=True)
            ho_ref[band, :] = (centered * lax.rsqrt(variance + LN_EPS) * gb_ref[0:1, :] + gb_ref[1:2, :]).astype(BF16)


def pair_stride(width):
    return -(-(-(-width // 128)) // 8) * 8


def layer_block(layer, last, h, positions, cs, x, gb, w_qkv, k_cache, v_cache, w_up, w_down, w_out):
    rows, width = x.shape
    head_dim, seq_len = k_cache.shape[2:]
    ff = w_up.shape[2]
    total = w_qkv.shape[2]
    tail = total - total // CHUNK * CHUNK
    n_up = -(-ff // CHUNK)
    n_dn = -(-width // CHUNK)
    size = lax.axis_size("tp")
    vmem = pl.BlockSpec(memory_space=pltpu.VMEM)
    smem = pl.BlockSpec(memory_space=pltpu.SMEM)
    hbm = pl.BlockSpec(memory_space=pl.ANY)
    row_shape = jax.ShapeDtypeStruct((rows, width), BF16)
    outs = [
        jax.ShapeDtypeStruct((size * rows, width), BF16),
        jax.ShapeDtypeStruct((rows, 2 * head_dim), BF16),
        row_shape,
    ]
    norm_scratch = [pltpu.VMEM((rows, width), BF16)]
    if not last:
        outs.append(row_shape)
        norm_scratch = []
    return pl.pallas_call(
        functools.partial(layer_kernel, layer, last),
        out_shape=outs,
        in_specs=[vmem, smem, vmem, hbm, vmem] + [hbm] * 6,
        out_specs=[hbm] + [vmem] * (len(outs) - 1),
        scratch_shapes=norm_scratch + [
            pltpu.VMEM((width, ff), BF16),
            pltpu.VMEM((width, tail), BF16),
            pltpu.VMEM((rows, 2 * head_dim), F32),
            pltpu.VMEM((2 * rows, width), BF16),
            pltpu.VMEM((2 * rows, ff), BF16),
            pltpu.VMEM((2 * rows, CHUNK), F32),
            pltpu.VMEM((2, rows, CHUNK), F32),
            pltpu.VMEM((4, rows, CHUNK), BF16),
            pltpu.VMEM((2 * n_dn + 1, rows, CHUNK), BF16),
            pltpu.VMEM((3 * n_dn + 1, rows, CHUNK), BF16),
            pltpu.VMEM((3, n_dn, rows, CHUNK), BF16),
            pltpu.SemaphoreType.DMA((QKV_SLOTS,)),
            pltpu.SemaphoreType.DMA,
            pltpu.SemaphoreType.DMA((2, CACHE_SLOTS)),
            pltpu.SemaphoreType.DMA,
            pltpu.SemaphoreType.DMA((2, 3)),
            pltpu.SemaphoreType.DMA((2, 3)),
            pltpu.SemaphoreType.DMA((5,)),
            pltpu.SemaphoreType.DMA((5,)),
            pltpu.SemaphoreType.DMA((n_up,)),
            pltpu.SemaphoreType.DMA((n_dn,)),
            pltpu.SemaphoreType.DMA((4,)),
            pltpu.SemaphoreType.DMA((4,)),
            pltpu.SemaphoreType.DMA,
            pltpu.SemaphoreType.DMA((4,)),
            pltpu.SemaphoreType.DMA((4, n_dn)),
            pltpu.SemaphoreType.DMA((5, n_dn)),
            pltpu.SemaphoreType.DMA((5, n_dn)),
        ],
        compiler_params=pltpu.CompilerParams(
            collective_id=layer, has_side_effects=True, vmem_limit_bytes=67_043_328),
    )(h, positions, cs, x, gb, w_qkv, k_cache, v_cache, w_up, w_down, w_out)


def layer_norm(rows_in, gamma_row, beta_row):
    values = rows_in.astype(F32)
    row_mean = jnp.mean(values, axis=-1, keepdims=True)
    centered = values - row_mean
    variance = jnp.mean(centered * centered, axis=-1, keepdims=True)
    return (centered * lax.rsqrt(variance + LN_EPS) * gamma_row + beta_row).astype(BF16)


def device_layers(hidden, positions, ln_gamma, ln_beta, w_qkv, w_out, w_up, w_down, k_cache, v_cache):
    layers = w_qkv.shape[0]
    seq_len, head_dim = k_cache.shape[2:]
    half_dim = head_dim // 2
    inv_freq = 1.0 / (ROPE_BASE ** (jnp.arange(half_dim, dtype=F32) * (2.0 / head_dim)))
    angles = positions.astype(F32)[:, None] * inv_freq[None, :]
    cos_table = jnp.cos(angles)
    sin_table = jnp.sin(angles)
    cs = jnp.stack([jnp.tile(cos_table, (1, 4)), jnp.tile(jnp.concatenate([-sin_table, sin_table], axis=1), (1, 2))])
    k_turned = jnp.swapaxes(k_cache, 2, 3)
    v_turned = jnp.swapaxes(v_cache, 2, 3)
    x = hidden
    normed = layer_norm(x, ln_gamma[0], ln_beta[0])
    rows_new = []
    for layer in range(layers):
        last = layer == layers - 1
        nxt = layer if last else layer + 1
        gb = jnp.stack([ln_gamma[nxt], ln_beta[nxt]])
        outs = layer_block(layer, last, normed, positions, cs, x, gb, w_qkv, k_turned, v_turned, w_up, w_down, w_out)
        rows_new.append(outs[1])
        x = outs[2]
        if not last:
            normed = outs[3]
    seq_ids = jnp.arange(seq_len, dtype=jnp.int32)
    mask = (seq_ids[None, :] == positions[:, None])[None, :, :, None]
    rows_new = jnp.stack(rows_new)[:, :, None, :]
    k_new = jnp.where(mask, rows_new[..., :head_dim], k_cache)
    v_new = jnp.where(mask, rows_new[..., head_dim:], v_cache)
    return x, k_new, v_new


def solution(mesh):
    row_spec = P(('dp', 'tp'), None)
    cache_spec = P(None, ('dp', 'tp'), None, None)
    in_specs = (row_spec, P(('dp', 'tp')), P(), P(), P(), P(), P(None, None, 'tp'), P(None, 'tp', None), cache_spec, cache_spec)
    return jax.shard_map(device_layers, mesh=mesh, in_specs=in_specs, out_specs=(row_spec, cache_spec, cache_spec), check_vma=False)
```
